32 devices in a mesh: gx: 4 (over x, core), gy: 4 (over z), gz: 2 (over y).
Axes of the slice: x: 2, y: 2, z: 4, core: 2. Of those that a mesh axis runs over, the one named last changes fastest.
Arguments:
- kappa: float32 [5, 5, 5, 4, 4, 128], P(None, None, None, 'gx', 'gy', 'gz'), may hold values from 0.2 to 5
- source: float32 [5, 5, 5, 4, 4, 128], P(None, None, None, 'gx', 'gy', 'gz'), may hold values from -24 to 24
Outputs:
- solution: float32 [16, 16, 512], P('gx', 'gy', 'gz')
- residual: float32 [16, 16, 512], P('gx', 'gy', 'gz')
The draws below stay inside these ranges and needn't reach their ends.
All inputs are finite; a program needn't handle non-finite values.
Results may differ from the reference program's by a relative error of at most 0.0003.
Values sent between devices are 32-bit elements; how exact they have to be, the bound alone decides.
No kernel may reach another device: no remote copies, remote signals or barrier semaphores. Data moves between devices by JAX's collectives and lax.ppermute only.
A program may use at most 64 MiB of HBM per device.

```python
import math
import jax
import jax.numpy as jnp
import numpy as np
from jax import lax

POLY_DEGREE = 4
LEVELS = 3
SWEEPS = 2
ELEMENTS_X = 4
ELEMENTS_Y = 4
ELEMENTS_Z = 128


def level_of(own_key, shape, pieces, smallest, top_value):
    def one(position, blocks):
        steps = jax.random.uniform(jax.random.fold_in(jax.random.fold_in(own_key, 6), position), (blocks,), jnp.float32, smallest / len(pieces), top_value / len(pieces))
        return jnp.repeat(jnp.exp(steps), shape[position] // blocks).reshape((-1,) + (1,) * (len(shape) - position - 1))

    gain = one(*pieces[0])
    for cut in pieces[1:]:
        gain = gain * one(*cut)
    return gain


def bell_draw(own_key, dims, scale, reach, cuts=(), kind=jnp.bfloat16):
    result = jax.random.normal(own_key, dims, jnp.float32) * scale
    if len(cuts) > 0:
        result = level_of(own_key, dims, cuts, -0.22, 0.18) * result
    return jnp.clip(result, min=-reach, max=reach).astype(kind)


def setup_inputs(seed: int = 0) -> dict:
    splits = jax.random.split(jax.random.key(seed), 3)
    kappa = jnp.clip(jnp.exp(math.log(5.0) - 3.218876 * jax.random.uniform(splits[0], (POLY_DEGREE + 1, POLY_DEGREE + 1, POLY_DEGREE + 1, ELEMENTS_X, ELEMENTS_Y, ELEMENTS_Z), jnp.float32) ** level_of(splits[0], (POLY_DEGREE + 1, POLY_DEGREE + 1, POLY_DEGREE + 1, ELEMENTS_X, ELEMENTS_Y, ELEMENTS_Z), ((3, 4), (4, 4), (5, 2)), -0.2, 0.2)), 0.2, 5.0)
    source = bell_draw(splits[1], (POLY_DEGREE + 1, POLY_DEGREE + 1, POLY_DEGREE + 1, ELEMENTS_X, ELEMENTS_Y, ELEMENTS_Z), 4.0, 24.0, ((3, 4), (4, 4), (5, 2)), jnp.float32)
    return dict(kappa=kappa, source=source)


relax_weight = 0.6

def gll_tables():
    points = np.array([-1.0, -math.sqrt(3.0 / 7.0), 0.0, math.sqrt(3.0 / 7.0), 1.0])
    quad_weights = np.array([0.1, 49.0 / 90.0, 32.0 / 45.0, 49.0 / 90.0, 0.1])
    bary = np.array([np.prod([points[i] - points[k] for k in range(5) if k != i]) for i in range(5)])
    deriv = np.zeros((5, 5))
    for i in range(5):
        for j in range(5):
            if i != j:
                deriv[i, j] = bary[i] / (bary[j] * (points[i] - points[j]))
    for i in range(5):
        deriv[i, i] = -np.sum(deriv[i])
    return (jnp.asarray(points, jnp.float32), jnp.asarray(quad_weights, jnp.float32), jnp.asarray(deriv, jnp.float32))

def split_first(values):
    count = (values.shape[0] - 1) // 4
    lower = jnp.swapaxes(values[:-1].reshape((count, 4) + values.shape[1:]), 0, 1)
    return jnp.concatenate([lower, values[4::4][None]], axis=0)

def merge_first(block):
    count = block.shape[1]
    rest = block.shape[2:]
    lower = jnp.swapaxes(block[:4], 0, 1).reshape((4 * count,) + rest)
    tail = jnp.concatenate([jnp.zeros((count, 3) + rest, block.dtype), block[4][:, None]], axis=1)
    tail = tail.reshape((4 * count,) + rest)
    spare = [(0, 0)] * len(rest)
    return jnp.pad(lower, [(0, 1)] + spare) + jnp.pad(tail, [(1, 0)] + spare)

def element_view(field):
    element_portion = split_first(field)
    element_portion = split_first(jnp.moveaxis(element_portion, 2, 0))
    element_portion = split_first(jnp.moveaxis(element_portion, 4, 0))
    return jnp.transpose(element_portion, (4, 2, 0, 5, 3, 1))

def node_sum(block):
    element_portion = jnp.transpose(block, (2, 5, 1, 4, 0, 3))
    element_portion = jnp.moveaxis(merge_first(element_portion), 0, 4)
    element_portion = jnp.moveaxis(merge_first(element_portion), 0, 2)
    return merge_first(element_portion)

def stiffness_terms(field, weighted, deriv):
    highest = lax.Precision.HIGHEST
    local = element_view(field)
    grad_x = jnp.einsum('ia,abcxyz->ibcxyz', deriv, local, precision=highest)
    grad_y = jnp.einsum('jb,abcxyz->ajcxyz', deriv, local, precision=highest)
    grad_z = jnp.einsum('kc,abcxyz->abkxyz', deriv, local, precision=highest)
    back = jnp.einsum('ia,ibcxyz->abcxyz', deriv, weighted * grad_x, precision=highest)
    back = back + jnp.einsum('jb,ajcxyz->abcxyz', deriv, weighted * grad_y, precision=highest)
    back = back + jnp.einsum('kc,abkxyz->abcxyz', deriv, weighted * grad_z, precision=highest)
    return node_sum(back)

def mass_pair(paired, width):
    return jnp.stack([width / 6.0 * (2.0 * paired[0] + paired[1]), width / 6.0 * (paired[0] + 2.0 * paired[1])])

def stiff_pair(paired, width):
    slope = (paired[0] - paired[1]) / width
    return jnp.stack([slope, -slope])

def lor_terms(field, coeff, spacing):
    width_x, width_y, width_z = spacing
    zpairs = jnp.stack([field[:, :, :-1], field[:, :, 1:]])
    zmass = mass_pair(zpairs, width_z)
    stiffness_along_z = stiff_pair(zpairs, width_z)
    ymass = jnp.stack([zmass[:, :, :-1], zmass[:, :, 1:]])
    ystiff = jnp.stack([stiffness_along_z[:, :, :-1], stiffness_along_z[:, :, 1:]])
    column_y = width_y[:, None]
    first = mass_pair(ymass, column_y)
    second = stiff_pair(ymass, column_y) + mass_pair(ystiff, column_y)
    column_x = width_x[:, None, None]
    xfirst = jnp.stack([first[:, :, :-1], first[:, :, 1:]])
    xsecond = jnp.stack([second[:, :, :-1], second[:, :, 1:]])
    cells = (stiff_pair(xfirst, column_x) + mass_pair(xsecond, column_x)) * coeff
    total = jnp.zeros(field.shape, jnp.float32)
    for a in range(2):
        for b in range(2):
            for c in range(2):
                total = total + jnp.pad(cells[a, b, c], ((a, 1 - a), (b, 1 - b), (c, 1 - c)))
    return total

def lor_diagonal(coeff, spacing):
    width_x = spacing[0][:, None, None]
    width_y = spacing[1][None, :, None]
    width_z = spacing[2][None, None, :]
    cells = coeff * (width_y * width_z / (9.0 * width_x) + width_x * width_z / (9.0 * width_y) + width_x * width_y / (9.0 * width_z))
    shape = tuple((n + 1 for n in coeff.shape))
    total = jnp.zeros(shape, jnp.float32)
    for a in range(2):
        for b in range(2):
            for c in range(2):
                total = total + jnp.pad(cells, ((a, 1 - a), (b, 1 - b), (c, 1 - c)))
    return total

def subcell_coefficient(kappa):
    averaged = 0.5 * (kappa[:-1] + kappa[1:])
    averaged = 0.5 * (averaged[:, :-1] + averaged[:, 1:])
    averaged = 0.5 * (averaged[:, :, :-1] + averaged[:, :, 1:])
    count_x, count_y, count_z = averaged.shape[3:]
    return jnp.transpose(averaged, (3, 0, 4, 1, 5, 2)).reshape(4 * count_x, 4 * count_y, 4 * count_z)

def coarsen(coeff):
    nx, ny, nz = coeff.shape
    return lax.optimization_barrier(jnp.mean(coeff.reshape(nx // 2, 2, ny // 2, 2, nz // 2, 2), axis=(1, 3, 5)))

def interp_weights(width):
    paired = width.reshape(-1, 2)
    span = paired[:, 0] + paired[:, 1]
    return (paired[:, 1] / span, paired[:, 0] / span)

def prolong_first(coarse, left, right):
    shape = (-1,) + (1,) * (coarse.ndim - 1)
    middle = left.reshape(shape) * coarse[:-1] + right.reshape(shape) * coarse[1:]
    woven = jnp.stack([coarse[:-1], middle], axis=1).reshape((2 * (coarse.shape[0] - 1),) + coarse.shape[1:])
    return jnp.concatenate([woven, coarse[-1:]], axis=0)

def restrict_first(fine, left, right):
    shape = (-1,) + (1,) * (fine.ndim - 1)
    middle = fine[1::2]
    spare = [(0, 0)] * (fine.ndim - 1)
    return fine[0::2] + jnp.pad(left.reshape(shape) * middle, [(0, 1)] + spare) + jnp.pad(right.reshape(shape) * middle, [(1, 0)] + spare)

def prolong(coarse, weight_sets):
    for axis in range(3):
        left, right = weight_sets[axis]
        coarse = jnp.moveaxis(prolong_first(jnp.moveaxis(coarse, axis, 0), left, right), 0, axis)
    return coarse

def restrict(fine, weight_sets):
    for axis in range(3):
        left, right = weight_sets[axis]
        fine = jnp.moveaxis(restrict_first(jnp.moveaxis(fine, axis, 0), left, right), 0, axis)
    return fine

def edge_mask(shape):
    masks = []
    for n in shape:
        index = jnp.arange(n + 1)
        masks.append(((index > 0) & (index < n)).astype(jnp.float32))
    return masks[0][:, None, None] * masks[1][None, :, None] * masks[2][None, None, :]

def cycle(level, forcing, levels):
    coeff, spacing, diag, mask, weight_sets = levels[level]
    guess = relax_weight * forcing / diag
    if level == LEVELS - 1:
        for sweep in range(SWEEPS - 1):
            guess = guess + relax_weight * (forcing - mask * lor_terms(guess, coeff, spacing)) / diag
        return guess
    defect = forcing - lor_terms(guess, coeff, spacing)
    coarse = levels[level + 1][3] * restrict(defect, weight_sets)
    guess = guess + prolong(cycle(level + 1, coarse, levels), weight_sets)
    return guess + relax_weight * (forcing - mask * lor_terms(guess, coeff, spacing)) / diag

def reference(kappa, source):
    points, quad_weights, deriv = gll_tables()
    cube = (quad_weights[:, None, None] * quad_weights[None, :, None] * quad_weights[None, None, :]).reshape(5, 5, 5, 1, 1, 1)
    weighted = kappa * cube
    counts = kappa.shape[3:]
    finest_mask = edge_mask([4 * c for c in counts])
    rhs = finest_mask * node_sum(cube * source)
    gaps = points[1:] - points[:-1]
    spacing = [jnp.tile(gaps, c) for c in counts]
    coeff = subcell_coefficient(kappa)
    levels = []
    for level in range(LEVELS):
        weight_sets = [interp_weights(h) for h in spacing] if level < LEVELS - 1 else None
        levels.append((coeff, spacing, lor_diagonal(coeff, spacing), edge_mask(coeff.shape), weight_sets))
        if level < LEVELS - 1:
            coeff = coarsen(coeff)
            spacing = [h.reshape(-1, 2).sum(axis=1) for h in spacing]

    def operator(field):
        return finest_mask * stiffness_terms(field, weighted, deriv)
    resid = rhs
    precond = cycle(0, resid, levels)
    rho_old = jnp.sum(resid * precond)
    direction = precond
    image = operator(direction)
    alpha = rho_old / jnp.sum(direction * image)
    iterate = alpha * direction
    resid = resid - alpha * image
    precond = cycle(0, resid, levels)
    rho_new = jnp.sum(resid * precond)
    direction = precond + rho_new / rho_old * direction
    image = operator(direction)
    alpha = rho_new / jnp.sum(direction * image)
    iterate = iterate + alpha * direction
    resid = resid - alpha * image
    return (iterate[1:, 1:, 1:], resid[1:, 1:, 1:])
```

```python
import math

import jax
import jax.numpy as jnp
import numpy as np
from jax import lax
from jax.experimental import pallas as pl
from jax.experimental.pallas import tpu as pltpu
from jax.sharding import PartitionSpec as P

LEVELS = 3


relax_weight = 0.6


def extended(cells, sides, width):
    for axis, dim in sides:
        count = lax.axis_size(axis)
        ends = count - 1
        head = lax.slice_in_dim(cells, 0, width, axis=dim)
        tail = lax.slice_in_dim(cells, cells.shape[dim] - width, cells.shape[dim], axis=dim)
        cells = jnp.concatenate(
            [
                lax.ppermute(tail, axis, [(i, (i + 1) % count) for i in range(ends)]),
                cells,
                lax.ppermute(head, axis, [((i + 1) % count, i) for i in range(ends)]),
            ],
            axis=dim,
        )
    return cells


def gll_tables():
    points = np.array([-1.0, -math.sqrt(3.0 / 7.0), 0.0, math.sqrt(3.0 / 7.0), 1.0])
    quad_weights = np.array([0.1, 49.0 / 90.0, 32.0 / 45.0, 49.0 / 90.0, 0.1])
    bary = np.array(
        [np.prod([points[i] - points[k] for k in range(5) if k != i]) for i in range(5)]
    )
    deriv = np.zeros((5, 5))
    for i in range(5):
        for j in range(5):
            if i != j:
                deriv[i, j] = bary[i] / (bary[j] * (points[i] - points[j]))
    for i in range(5):
        deriv[i, i] = -np.sum(deriv[i])
    return (
        jnp.asarray(points, jnp.float32),
        jnp.asarray(quad_weights, jnp.float32),
        jnp.asarray(deriv, jnp.float32),
    )


def split_first(values):
    count = (values.shape[0] - 1) // 4
    lower = jnp.swapaxes(values[:-1].reshape((count, 4) + values.shape[1:]), 0, 1)
    return jnp.concatenate([lower, values[4::4][None]], axis=0)


def merge_first(block):
    count = block.shape[1]
    rest = block.shape[2:]
    lower = jnp.swapaxes(block[:4], 0, 1).reshape((4 * count,) + rest)
    tail = jnp.concatenate([jnp.zeros((count, 3) + rest, block.dtype), block[4][:, None]], axis=1)
    tail = tail.reshape((4 * count,) + rest)
    spare = [(0, 0)] * len(rest)
    return jnp.pad(lower, [(0, 1)] + spare) + jnp.pad(tail, [(1, 0)] + spare)


def element_view(field):
    element_portion = split_first(field)
    element_portion = split_first(jnp.moveaxis(element_portion, 2, 0))
    element_portion = split_first(jnp.moveaxis(element_portion, 4, 0))
    return jnp.transpose(element_portion, (4, 2, 0, 5, 3, 1))


def node_sum(block):
    element_portion = jnp.transpose(block, (2, 5, 1, 4, 0, 3))
    element_portion = jnp.moveaxis(merge_first(element_portion), 0, 4)
    element_portion = jnp.moveaxis(merge_first(element_portion), 0, 2)
    return merge_first(element_portion)


def stiffness_terms(field, weighted, deriv):
    highest = lax.Precision.HIGHEST
    local = element_view(field)
    grad_x = jnp.einsum("ia,abcxyz->ibcxyz", deriv, local, precision=highest)
    grad_y = jnp.einsum("jb,abcxyz->ajcxyz", deriv, local, precision=highest)
    grad_z = jnp.einsum("kc,abcxyz->abkxyz", deriv, local, precision=highest)
    back = jnp.einsum("ia,ibcxyz->abcxyz", deriv, weighted * grad_x, precision=highest)
    back = back + jnp.einsum("jb,ajcxyz->abcxyz", deriv, weighted * grad_y, precision=highest)
    back = back + jnp.einsum("kc,abkxyz->abcxyz", deriv, weighted * grad_z, precision=highest)
    return node_sum(back)


def mass_pair(paired, width):
    return jnp.stack(
        [width / 6.0 * (2.0 * paired[0] + paired[1]), width / 6.0 * (paired[0] + 2.0 * paired[1])]
    )


def stiff_pair(paired, width):
    slope = (paired[0] - paired[1]) / width
    return jnp.stack([slope, -slope])


def lor_terms(field, coeff, spacing):
    width_x, width_y, width_z = spacing
    zpairs = jnp.stack([field[:, :, :-1], field[:, :, 1:]])
    zmass = mass_pair(zpairs, width_z)
    stiffness_along_z = stiff_pair(zpairs, width_z)
    ymass = jnp.stack([zmass[:, :, :-1], zmass[:, :, 1:]])
    ystiff = jnp.stack([stiffness_along_z[:, :, :-1], stiffness_along_z[:, :, 1:]])
    column_y = width_y[:, None]
    first = mass_pair(ymass, column_y)
    second = stiff_pair(ymass, column_y) + mass_pair(ystiff, column_y)
    column_x = width_x[:, None, None]
    xfirst = jnp.stack([first[:, :, :-1], first[:, :, 1:]])
    xsecond = jnp.stack([second[:, :, :-1], second[:, :, 1:]])
    cells = (stiff_pair(xfirst, column_x) + mass_pair(xsecond, column_x)) * coeff
    total = jnp.zeros(field.shape, jnp.float32)
    for a in range(2):
        for b in range(2):
            for c in range(2):
                total = total + jnp.pad(cells[a, b, c], ((a, 1 - a), (b, 1 - b), (c, 1 - c)))
    return total


def lor_diagonal(coeff, spacing):
    width_x = spacing[0][:, None, None]
    width_y = spacing[1][None, :, None]
    width_z = spacing[2][None, None, :]
    cells = coeff * (
        width_y * width_z / (9.0 * width_x)
        + width_x * width_z / (9.0 * width_y)
        + width_x * width_y / (9.0 * width_z)
    )
    shape = tuple((n + 1 for n in coeff.shape))
    total = jnp.zeros(shape, jnp.float32)
    for a in range(2):
        for b in range(2):
            for c in range(2):
                total = total + jnp.pad(cells, ((a, 1 - a), (b, 1 - b), (c, 1 - c)))
    return total


def subcell_coefficient(kappa):
    averaged = 0.5 * (kappa[:-1] + kappa[1:])
    averaged = 0.5 * (averaged[:, :-1] + averaged[:, 1:])
    averaged = 0.5 * (averaged[:, :, :-1] + averaged[:, :, 1:])
    count_x, count_y, count_z = averaged.shape[3:]
    return jnp.transpose(averaged, (3, 0, 4, 1, 5, 2)).reshape(
        4 * count_x, 4 * count_y, 4 * count_z
    )


def coarsen(coeff):
    nx, ny, nz = coeff.shape
    return jnp.mean(coeff.reshape(nx // 2, 2, ny // 2, 2, nz // 2, 2), axis=(1, 3, 5))


def interp_weights(width):
    paired = width.reshape(-1, 2)
    span = paired[:, 0] + paired[:, 1]
    return (paired[:, 1] / span, paired[:, 0] / span)


def prolong_first(coarse, left, right):
    shape = (-1,) + (1,) * (coarse.ndim - 1)
    middle = left.reshape(shape) * coarse[:-1] + right.reshape(shape) * coarse[1:]
    woven = jnp.stack([coarse[:-1], middle], axis=1).reshape(
        (2 * (coarse.shape[0] - 1),) + coarse.shape[1:]
    )
    return jnp.concatenate([woven, coarse[-1:]], axis=0)


def restrict_first(fine, left, right):
    shape = (-1,) + (1,) * (fine.ndim - 1)
    middle = fine[1::2]
    spare = [(0, 0)] * (fine.ndim - 1)
    return (
        fine[0::2]
        + jnp.pad(left.reshape(shape) * middle, [(0, 1)] + spare)
        + jnp.pad(right.reshape(shape) * middle, [(1, 0)] + spare)
    )


def prolong(coarse, weight_sets):
    for axis in range(3):
        left, right = weight_sets[axis]
        coarse = jnp.moveaxis(prolong_first(jnp.moveaxis(coarse, axis, 0), left, right), 0, axis)
    return coarse


def restrict(fine, weight_sets):
    for axis in range(3):
        left, right = weight_sets[axis]
        fine = jnp.moveaxis(restrict_first(jnp.moveaxis(fine, axis, 0), left, right), 0, axis)
    return fine


def collapse_leading(padded):
    inner = padded[1:-1]
    head = inner[0] + padded[0]
    tail = inner[-1] + padded[-1]
    return jnp.concatenate([head[None], inner[1:-1], tail[None]], axis=0)


def fold_axis(padded, axis):
    return jnp.moveaxis(collapse_leading(jnp.moveaxis(padded, axis, 0)), 0, axis)


def assemble(partial_value):
    padded = extended(partial_value, (("gx", 0), ("gy", 1), ("gz", 2)), 1)
    return fold_axis(fold_axis(fold_axis(padded, 0), 1), 2)


def side_mask(cells, position, devices):
    index = position * cells + jnp.arange(cells + 1)
    return ((index > 0) & (index < cells * devices)).astype(jnp.float32)


def block_mask(shape):
    mask_x = side_mask(shape[0], lax.axis_index("gx"), lax.axis_size("gx"))
    mask_y = side_mask(shape[1], lax.axis_index("gy"), lax.axis_size("gy"))
    mask_z = side_mask(shape[2], lax.axis_index("gz"), lax.axis_size("gz"))
    return mask_x[:, None, None] * mask_y[None, :, None] * mask_z[None, None, :]


def owned_mask(shape):
    sides = [(jnp.arange(n + 1) >= 1).astype(jnp.float32) for n in shape]
    return sides[0][:, None, None] * sides[1][None, :, None] * sides[2][None, None, :]


def cycle(level, forcing, levels):
    coeff, spacing, diag, mask, weight_sets, owned = levels[level]
    guess = relax_weight * forcing / diag
    if level == LEVELS - 1:
        guess = (
            guess
            + relax_weight * (forcing - mask * assemble(lor_terms(guess, coeff, spacing))) / diag
        )
        return guess
    defect = forcing * owned - lor_terms(guess, coeff, spacing)
    coarse = levels[level + 1][3] * assemble(restrict(defect, weight_sets))
    guess = guess + prolong(cycle(level + 1, coarse, levels), weight_sets)
    return (
        guess + relax_weight * (forcing - mask * assemble(lor_terms(guess, coeff, spacing))) / diag
    )


def inner_pair(resid, precond, image):
    local_rho = jnp.sum(resid[1:, 1:, 1:] * precond[1:, 1:, 1:])
    local_curv = jnp.sum(precond[1:, 1:, 1:] * image[1:, 1:, 1:])
    return lax.psum((local_rho, local_curv), ("gx", "gy", "gz"))


def body(kappa, source):
    points, quad_weights, deriv = gll_tables()
    cube = (
        quad_weights[:, None, None] * quad_weights[None, :, None] * quad_weights[None, None, :]
    ).reshape(5, 5, 5, 1, 1, 1)
    weighted = kappa * cube
    counts = kappa.shape[3:]
    finest_mask = block_mask([4 * c for c in counts])
    rhs = finest_mask * assemble(node_sum(cube * source))
    gaps = points[1:] - points[:-1]
    spacing = [jnp.tile(gaps, c) for c in counts]
    coeff = subcell_coefficient(kappa)
    levels = []
    for level in range(LEVELS):
        weight_sets = [interp_weights(h) for h in spacing] if level < LEVELS - 1 else None
        diag = assemble(lor_diagonal(coeff, spacing))
        levels.append(
            (coeff, spacing, diag, block_mask(coeff.shape), weight_sets, owned_mask(coeff.shape))
        )
        if level < LEVELS - 1:
            coeff = coarsen(coeff)
            spacing = [h.reshape(-1, 2).sum(axis=1) for h in spacing]

    def operator(field):
        return finest_mask * assemble(stiffness_terms(field, weighted, deriv))

    resid = rhs
    precond = cycle(0, resid, levels)
    image = operator(precond)
    rho_old, curv = inner_pair(resid, precond, image)
    alpha = rho_old / curv
    direction, along = (precond, image)
    iterate = alpha * direction
    resid = resid - alpha * along
    precond = cycle(0, resid, levels)
    image = operator(precond)
    rho_new, curv = inner_pair(resid, precond, image)
    ratio = rho_new / rho_old
    alpha = rho_new / (curv - ratio * rho_new / alpha)
    direction = precond + ratio * direction
    along = image + ratio * along
    iterate = iterate + alpha * direction
    resid = resid - alpha * along
    return (iterate[1:, 1:, 1:], resid[1:, 1:, 1:])


def exact_tables():
    points = np.array([-1.0, -math.sqrt(3.0 / 7.0), 0.0, math.sqrt(3.0 / 7.0), 1.0])
    quad_weights = np.array([0.1, 49.0 / 90.0, 32.0 / 45.0, 49.0 / 90.0, 0.1])
    bary = np.array(
        [np.prod([points[i] - points[k] for k in range(5) if k != i]) for i in range(5)]
    )
    deriv = np.zeros((5, 5))
    for i in range(5):
        for j in range(5):
            if i != j:
                deriv[i, j] = bary[i] / (bary[j] * (points[i] - points[j]))
    for i in range(5):
        deriv[i, i] = -np.sum(deriv[i])
    return points, quad_weights, deriv


def level_widths():
    points = exact_tables()[0]
    widths = [[float(h) for h in points[1:] - points[:-1]]]
    for _ in range(LEVELS - 1):
        last = widths[-1]
        widths.append([last[2 * i] + last[2 * i + 1] for i in range(len(last) // 2)])
    return widths


def cell_scales(hx, hy, hz):
    mass = lambda h, odd: h / 12.0 if odd else h / 4.0
    scales = {}
    for p in range(2):
        for q in range(2):
            for r in range(2):
                scale = 0.0
                if p:
                    scale += mass(hy, q) * mass(hz, r) / hx
                if q:
                    scale += mass(hx, p) * mass(hz, r) / hy
                if r:
                    scale += mass(hx, p) * mass(hy, q) / hz
                scales[p, q, r] = scale
    return scales


def iteration_kernel(place, gathered, x_out, r_out, weighted, full, part, c0, c1, c2,
                     d0, d1, d2, f1, f2, g1, p1, g2, p2, guess1, resid, precond, direction,
                     iterate, *, ny):
    rows, lanes = resid.shape[1:]
    blocks = 2 * rows
    stride = gathered.shape[0] // rows
    half = stride // 2
    points, quad, deriv = exact_tables()
    widths = level_widths()
    cells = [len(h) for h in widths]
    coeffs, diags = (c0, c1, c2), (d0, d1, d2)
    fulls, parts = (full, g1, g2), (part, p1, p2)

    sub = lax.broadcasted_iota(jnp.int32, (rows, lanes), 0)
    lane = lax.broadcasted_iota(jnp.int32, (rows, lanes), 1)
    masks = (
        (sub < rows - ny).astype(jnp.float32),
        (sub % ny < ny - 1).astype(jnp.float32),
        (lane < lanes - 1).astype(jnp.float32),
    )

    def before(tile, dim):
        if dim == 2:
            return pltpu.roll(tile, 1, 1)
        return pltpu.roll(tile, (ny, 1)[dim], 0)

    def after(tile, dim):
        if dim == 2:
            return pltpu.roll(tile, lanes - 1, 1)
        return pltpu.roll(tile, rows - (ny, 1)[dim], 0)

    def at(n, a, b, c):
        return (a * (n + 1) + b) * (n + 1) + c

    def own(n, a, b, c):
        return ((a - 1) * n + b - 1) * n + c - 1

    def inside(n, a, b, c, tile):
        for dim, offset in enumerate((a, b, c)):
            if offset == n:
                tile = tile * masks[dim]
        return tile

    def ghosts(ref, n):
        for a in range(1, n + 1):
            for b in range(1, n + 1):
                ref[at(n, a, b, 0)] = before(ref[at(n, a, b, n)], 2)
            for c in range(n + 1):
                ref[at(n, a, 0, c)] = before(ref[at(n, a, n, c)], 1)
        for b in range(n + 1):
            for c in range(n + 1):
                ref[at(n, 0, b, c)] = before(ref[at(n, n, b, c)], 0)

    def fold(ref, n):
        for a in range(n + 1):
            for b in range(n + 1):
                ref[at(n, a, b, n)] += after(ref[at(n, a, b, 0)], 2)
            for c in range(1, n + 1):
                ref[at(n, a, n, c)] += after(ref[at(n, a, 0, c)], 1)
        for b in range(1, n + 1):
            for c in range(1, n + 1):
                ref[at(n, n, b, c)] += after(ref[at(n, 0, b, c)], 0)

    def owned(n):
        for a in range(1, n + 1):
            for b in range(1, n + 1):
                for c in range(1, n + 1):
                    yield a, b, c

    def lor(level):
        n, h = cells[level], widths[level]
        src, dst, coeff = fulls[level], parts[level], coeffs[level]
        ghosts(src, n)
        for b in range(n):
            for c in range(n):
                carried = None
                face = None
                for a in range(n + 1):
                    u = [[src[at(n, a, b + i, c + k)] for k in range(2)] for i in range(2)]
                    sums = [u[i][1] + u[i][0] for i in range(2)]
                    difs = [u[i][1] - u[i][0] for i in range(2)]
                    now = {
                        (0, 0): sums[1] + sums[0],
                        (1, 0): sums[1] - sums[0],
                        (0, 1): difs[1] + difs[0],
                        (1, 1): difs[1] - difs[0],
                    }
                    lower = {}
                    upper = {}
                    if a > 0:
                        scales = cell_scales(h[a - 1], h[b], h[c])
                        k = coeff[own(n, a, b + 1, c + 1)]
                        for key in now:
                            odd = ((now[key] - face[key]) * scales[(1,) + key]) * k
                            if key == (0, 0):
                                lower[key], upper[key] = -odd, odd
                            else:
                                even = ((now[key] + face[key]) * scales[(0,) + key]) * k
                                lower[key], upper[key] = even - odd, even + odd
                        total = {
                            key: lower[key] if carried is None else lower[key] + carried[key]
                            for key in now
                        }
                        spread(dst, n, a - 1, b, c, total)
                    face = now
                    carried = upper if a > 0 else None
                spread(dst, n, n, b, c, carried)
        fold(dst, n)

    def spread(dst, n, a, b, c, total):
        s1 = total[0, 0] + total[1, 0]
        s0 = total[0, 0] - total[1, 0]
        d1_ = total[0, 1] + total[1, 1]
        d0_ = total[0, 1] - total[1, 1]
        for i, s, d in ((0, s0, d0_), (1, s1, d1_)):
            for k, value in ((0, s - d), (1, s + d)):
                spot = at(n, a, b + i, c + k)
                if (i == 1 or b == 0) and (k == 1 or c == 0):
                    dst[spot] = value
                else:
                    dst[spot] += value

    def diagonal(level):
        n, h = cells[level], widths[level]
        dst, coeff = parts[level], coeffs[level]
        tiles = {}
        for a in range(n):
            for b in range(n):
                for c in range(n):
                    hx, hy, hz = h[a], h[b], h[c]
                    scale = hy * hz / (9 * hx) + hx * hz / (9 * hy) + hx * hy / (9 * hz)
                    tile = coeff[own(n, a + 1, b + 1, c + 1)] * scale
                    for i in range(2):
                        for j in range(2):
                            for k in range(2):
                                spot = at(n, a + i, b + j, c + k)
                                first = (i or a == 0) and (j or b == 0) and (k or c == 0)
                                if first:
                                    dst[spot] = tile
                                else:
                                    dst[spot] += tile
        fold(dst, n)
        for a, b, c in owned(n):
            diags[level][own(n, a, b, c)] = relax_weight / dst[at(n, a, b, c)]

    def pair_weights(level):
        h = widths[level]
        spans = [(h[2 * i], h[2 * i + 1]) for i in range(len(h) // 2)]
        return [q / (p + q) for p, q in spans], [p / (p + q) for p, q in spans]

    def restrict_to(level, defect, target):
        n = cells[level]
        m = n // 2
        left, right = pair_weights(level)

        def line(values, dim):
            result = []
            for o in range(1, m + 1):
                beyond = values[2 * o] if o < m else after(values[0], dim)
                result.append(
                    values[2 * o - 1] + right[o - 1] * values[2 * o - 2] + left[o % m] * beyond
                )
            return result

        slabs = []
        for a in range(1, n + 1):
            lines = [line([defect(a, b, c) for c in range(1, n + 1)], 2) for b in range(1, n + 1)]
            turned = [line([lines[b][c] for b in range(n)], 1) for c in range(m)]
            slabs.append(turned)
        for c in range(m):
            for b in range(m):
                out = line([slabs[a][c][b] for a in range(n)], 0)
                for a in range(m):
                    target[own(m, a + 1, b + 1, c + 1)] = inside(m, a + 1, b + 1, c + 1, out[a])

    def prolong_from(level, add):
        n = cells[level]
        m = n // 2
        left, right = pair_weights(level)
        src = fulls[level + 1]
        ghosts(src, m)

        def line(values):
            result = []
            for o in range(1, m + 1):
                result.append(left[o - 1] * values[o - 1] + right[o - 1] * values[o])
                result.append(values[o])
            return result

        slabs = []
        for a in range(m + 1):
            lines = [line([src[at(m, a, b, c)] for c in range(m + 1)]) for b in range(m + 1)]
            slabs.append([line([lines[b][c] for b in range(m + 1)]) for c in range(n)])
        for c in range(n):
            for b in range(n):
                out = line([slabs[a][c][b] for a in range(m + 1)])
                for a in range(n):
                    add(a + 1, b + 1, c + 1, out[a])

    def cycle_at(level, forcing, store):
        n = cells[level]
        src, dst, diag = fulls[level], parts[level], diags[level]
        for a, b, c in owned(n):
            spot = own(n, a, b, c)
            src[at(n, a, b, c)] = forcing[spot] * diag[spot]
        lor(level)
        if level < LEVELS - 1:
            restrict_to(
                level,
                lambda a, b, c: forcing[own(n, a, b, c)] - dst[at(n, a, b, c)],
                (f1, f2)[level],
            )

            def leave(a, b, c, tile):
                fulls[level + 1][at(n // 2, a, b, c)] = tile

            cycle_at(level + 1, (f1, f2)[level], leave)

            def add(a, b, c, tile):
                src[at(n, a, b, c)] += tile

            prolong_from(level, add)
            lor(level)
        for a, b, c in owned(n):
            spot = own(n, a, b, c)
            change = inside(n, a, b, c, (forcing[spot] - dst[at(n, a, b, c)]) * diag[spot])
            store(a, b, c, src[at(n, a, b, c)] + change)

    def derive(u):
        e = [u[0] + u[4], u[1] + u[3], u[2]]
        o = [u[0] - u[4], u[1] - u[3]]
        odd = []
        even = []
        for i in range(2):
            odd.append(sum(
                e[j] * float((deriv[i, j] + deriv[i, 4 - j]) / 2 if j < 2 else deriv[i, 2])
                for j in range(3)
            ))
        for i in range(3):
            even.append(sum(o[j] * float((deriv[i, j] - deriv[i, 4 - j]) / 2) for j in range(2)))
        return [even[0] + odd[0], even[1] + odd[1], even[2], even[1] - odd[1], even[0] - odd[0]]

    def derive_back(g):
        e = [g[0] + g[4], g[1] + g[3], g[2]]
        o = [g[0] - g[4], g[1] - g[3]]
        odd = []
        even = []
        for a in range(2):
            odd.append(sum(
                e[j] * float((deriv[j, a] + deriv[4 - j, a]) / 2 if j < 2 else deriv[2, a])
                for j in range(3)
            ))
        for a in range(3):
            even.append(sum(o[j] * float((deriv[j, a] - deriv[4 - j, a]) / 2) for j in range(2)))
        return [even[0] + odd[0], even[1] + odd[1], even[2], even[1] - odd[1], even[0] - odd[0]]

    def stiffness():
        ghosts(full, 4)

        def run(spots, first):
            grad = derive([full[s] for s in spots])
            back = derive_back([grad[i] * weighted[s] for i, s in enumerate(spots)])
            for s, value in zip(spots, back):
                if first:
                    part[s] = value
                else:
                    part[s] += value

        def outer(i, carry):
            for k in range(5):
                run([25 * i + 5 * k + t for t in range(5)], True)
            for k in range(5):
                run([25 * i + 5 * t + k for t in range(5)], False)
            return carry

        def along(i, carry):
            for k in range(5):
                run([25 * t + 5 * i + k for t in range(5)], False)
            return carry

        lax.fori_loop(0, 5, outer, 0)
        lax.fori_loop(0, 5, along, 0)
        fold(part, 4)

    low = lane < lanes // 2
    for a in range(5):
        for b in range(5):
            for c in range(5):
                spot = 25 * a + 5 * b + c
                first = gathered[pl.ds(spot, rows, stride=stride), :]
                second = gathered[pl.ds(half + spot, rows, stride=stride), :]
                cube = float(quad[a] * quad[b] * quad[c])
                full[spot] = jnp.where(low, first, pltpu.roll(second, lanes // 2, 1))
                part[spot] = jnp.where(low, pltpu.roll(first, lanes // 2, 1), second) * cube
                weighted[spot] = full[spot] * cube
    fold(part, 4)
    for a, b, c in owned(4):
        resid[own(4, a, b, c)] = inside(4, a, b, c, part[at(4, a, b, c)])
    for a in range(4):
        for b in range(4):
            plane = [
                (full[at(4, a, b, c)] + full[at(4, a + 1, b, c)])
                + (full[at(4, a, b + 1, c)] + full[at(4, a + 1, b + 1, c)])
                for c in range(5)
            ]
            for c in range(4):
                c0[own(4, a + 1, b + 1, c + 1)] = (plane[c] + plane[c + 1]) * 0.125
    for level in range(LEVELS - 1):
        m = cells[level + 1]
        for a, b, c in owned(m):
            total = None
            for i in range(2):
                for j in range(2):
                    for k in range(2):
                        tile = coeffs[level][
                            own(2 * m, 2 * a - i, 2 * b - j, 2 * c - k)
                        ]
                        total = tile if total is None else total + tile
            coeffs[level + 1][own(m, a, b, c)] = total * 0.125
    for level in range(LEVELS):
        diagonal(level)

    direction[...] = jnp.zeros_like(direction)
    iterate[...] = jnp.zeros_like(iterate)

    def settle(a, b, c, tile):
        precond[own(4, a, b, c)] = tile

    def product(tiles):
        total = None
        for tile in tiles:
            total = tile if total is None else total + tile
        return jnp.sum(jnp.sum(total, axis=0, keepdims=True), axis=1, keepdims=True)

    def step(number, rho_old):
        cycle_at(0, resid, settle)
        rho = product(resid[i] * precond[i] for i in range(64))
        ratio = jnp.where(number == 0, 0.0, rho / rho_old)
        for a, b, c in owned(4):
            spot = own(4, a, b, c)
            value = precond[spot] + ratio * direction[spot]
            direction[spot] = value
            full[at(4, a, b, c)] = value
        stiffness()
        curv = None
        for a, b, c in owned(4):
            image = inside(4, a, b, c, part[at(4, a, b, c)])
            precond[own(4, a, b, c)] = image
            term = direction[own(4, a, b, c)] * image
            curv = term if curv is None else curv + term
        alpha = rho / product([curv])
        for i in range(64):
            iterate[i] += alpha * direction[i]
            resid[i] -= alpha * precond[i]
        return rho

    lax.fori_loop(0, 2, step, jnp.ones((1, 1), jnp.float32))

    row = place[0]
    start = place[1]
    width = x_out.shape[1]
    ez = lax.broadcasted_iota(jnp.int32, (lanes, width), 0)
    spot_z = lax.broadcasted_iota(jnp.int32, (lanes, width), 1)
    for out, ref in ((x_out, iterate), (r_out, resid)):
        total = jnp.zeros((16, width), jnp.float32)
        for c in range(4):
            pick = (spot_z == 4 * (ez - start) + c).astype(jnp.float32)
            lines = jnp.concatenate(
                [ref[4 * ab + c, pl.ds(row, 1), :] for ab in range(16)], axis=0
            )
            total = total + jnp.dot(
                lines, pick, precision=lax.Precision.HIGHEST,
                preferred_element_type=jnp.float32,
            )
        out[...] = total


def whole_body(kappa, source):
    nx, ny = lax.axis_size("gx"), lax.axis_size("gy")
    rows, lanes = nx * ny, 2 * kappa.shape[5]
    packed = jnp.concatenate([kappa.reshape(125, -1), source.reshape(125, -1)], axis=1)
    packed = jnp.pad(packed, ((0, 3), (0, 0)))
    gathered = lax.all_gather(packed, ("gx", "gy", "gz"), axis=0, tiled=True)
    place = jnp.stack([
        lax.axis_index("gx") * ny + lax.axis_index("gy"),
        lax.axis_index("gz") * kappa.shape[5],
    ]).astype(jnp.int32)

    def tiles(count):
        return pltpu.VMEM((count, rows, lanes), jnp.float32)

    counts = [125, 125, 125, 64, 8, 1, 64, 8, 1, 8, 1, 27, 27, 8, 8, 8, 64, 64, 64, 64]
    width = 2 * lanes
    shape = jax.ShapeDtypeStruct((16, width), jnp.float32)
    vmem = pl.BlockSpec(memory_space=pltpu.VMEM)
    outs = pl.pallas_call(
        lambda *refs: iteration_kernel(*refs, ny=ny),
        out_shape=(shape, shape),
        in_specs=[pl.BlockSpec(memory_space=pltpu.SMEM), vmem],
        out_specs=(vmem, vmem),
        scratch_shapes=[tiles(n) for n in counts],
        compiler_params=pltpu.CompilerParams(vmem_limit_bytes=40 * 2**20),
        name="whole_iteration",
    )(place, gathered)
    return tuple(o.reshape(4, 4, width) for o in outs)


def fits_whole(kappa, mesh):
    sizes = mesh.shape
    rows = sizes["gx"] * sizes["gy"]
    one_column = kappa.shape[3] == sizes["gx"] and kappa.shape[4] == sizes["gy"]
    lanes = kappa.shape[5]
    return (
        one_column
        and sizes["gz"] == 2
        and rows % 8 == 0
        and lanes % 128 == 0
        and rows * lanes <= 16 * 128
    )


def solution(mesh):
    placed = (P(None, None, None, "gx", "gy", "gz"), P(None, None, None, "gx", "gy", "gz"))

    def run(kappa, source):
        return jax.shard_map(
            whole_body if fits_whole(kappa, mesh) else body,
            mesh=mesh,
            in_specs=placed,
            out_specs=(P("gx", "gy", "gz"), P("gx", "gy", "gz")),
            check_vma=False,
        )(kappa, source)

    return run
```

```python
import math

import jax
import jax.numpy as jnp
import numpy as np
from jax import lax
from jax.experimental import pallas as pl
from jax.experimental.pallas import tpu as pltpu
from jax.sharding import PartitionSpec as P

LEVELS = 3


relax_weight = 0.6


def extended(cells, sides, width):
    for axis, dim in sides:
        count = lax.axis_size(axis)
        ends = count - 1
        head = lax.slice_in_dim(cells, 0, width, axis=dim)
        tail = lax.slice_in_dim(cells, cells.shape[dim] - width, cells.shape[dim], axis=dim)
        cells = jnp.concatenate(
            [
                lax.ppermute(tail, axis, [(i, (i + 1) % count) for i in range(ends)]),
                cells,
                lax.ppermute(head, axis, [((i + 1) % count, i) for i in range(ends)]),
            ],
            axis=dim,
        )
    return cells


def gll_tables():
    points = np.array([-1.0, -math.sqrt(3.0 / 7.0), 0.0, math.sqrt(3.0 / 7.0), 1.0])
    quad_weights = np.array([0.1, 49.0 / 90.0, 32.0 / 45.0, 49.0 / 90.0, 0.1])
    bary = np.array(
        [np.prod([points[i] - points[k] for k in range(5) if k != i]) for i in range(5)]
    )
    deriv = np.zeros((5, 5))
    for i in range(5):
        for j in range(5):
            if i != j:
                deriv[i, j] = bary[i] / (bary[j] * (points[i] - points[j]))
    for i in range(5):
        deriv[i, i] = -np.sum(deriv[i])
    return (
        jnp.asarray(points, jnp.float32),
        jnp.asarray(quad_weights, jnp.float32),
        jnp.asarray(deriv, jnp.float32),
    )


def split_first(values):
    count = (values.shape[0] - 1) // 4
    lower = jnp.swapaxes(values[:-1].reshape((count, 4) + values.shape[1:]), 0, 1)
    return jnp.concatenate([lower, values[4::4][None]], axis=0)


def merge_first(block):
    count = block.shape[1]
    rest = block.shape[2:]
    lower = jnp.swapaxes(block[:4], 0, 1).reshape((4 * count,) + rest)
    tail = jnp.concatenate([jnp.zeros((count, 3) + rest, block.dtype), block[4][:, None]], axis=1)
    tail = tail.reshape((4 * count,) + rest)
    spare = [(0, 0)] * len(rest)
    return jnp.pad(lower, [(0, 1)] + spare) + jnp.pad(tail, [(1, 0)] + spare)


def element_view(field):
    element_portion = split_first(field)
    element_portion = split_first(jnp.moveaxis(element_portion, 2, 0))
    element_portion = split_first(jnp.moveaxis(element_portion, 4, 0))
    return jnp.transpose(element_portion, (4, 2, 0, 5, 3, 1))


def node_sum(block):
    element_portion = jnp.transpose(block, (2, 5, 1, 4, 0, 3))
    element_portion = jnp.moveaxis(merge_first(element_portion), 0, 4)
    element_portion = jnp.moveaxis(merge_first(element_portion), 0, 2)
    return merge_first(element_portion)


def stiffness_terms(field, weighted, deriv):
    highest = lax.Precision.HIGHEST
    local = element_view(field)
    grad_x = jnp.einsum("ia,abcxyz->ibcxyz", deriv, local, precision=highest)
    grad_y = jnp.einsum("jb,abcxyz->ajcxyz", deriv, local, precision=highest)
    grad_z = jnp.einsum("kc,abcxyz->abkxyz", deriv, local, precision=highest)
    back = jnp.einsum("ia,ibcxyz->abcxyz", deriv, weighted * grad_x, precision=highest)
    back = back + jnp.einsum("jb,ajcxyz->abcxyz", deriv, weighted * grad_y, precision=highest)
    back = back + jnp.einsum("kc,abkxyz->abcxyz", deriv, weighted * grad_z, precision=highest)
    return node_sum(back)


def mass_pair(paired, width):
    return jnp.stack(
        [width / 6.0 * (2.0 * paired[0] + paired[1]), width / 6.0 * (paired[0] + 2.0 * paired[1])]
    )


def stiff_pair(paired, width):
    slope = (paired[0] - paired[1]) / width
    return jnp.stack([slope, -slope])


def lor_terms(field, coeff, spacing):
    width_x, width_y, width_z = spacing
    zpairs = jnp.stack([field[:, :, :-1], field[:, :, 1:]])
    zmass = mass_pair(zpairs, width_z)
    stiffness_along_z = stiff_pair(zpairs, width_z)
    ymass = jnp.stack([zmass[:, :, :-1], zmass[:, :, 1:]])
    ystiff = jnp.stack([stiffness_along_z[:, :, :-1], stiffness_along_z[:, :, 1:]])
    column_y = width_y[:, None]
    first = mass_pair(ymass, column_y)
    second = stiff_pair(ymass, column_y) + mass_pair(ystiff, column_y)
    column_x = width_x[:, None, None]
    xfirst = jnp.stack([first[:, :, :-1], first[:, :, 1:]])
    xsecond = jnp.stack([second[:, :, :-1], second[:, :, 1:]])
    cells = (stiff_pair(xfirst, column_x) + mass_pair(xsecond, column_x)) * coeff
    total = jnp.zeros(field.shape, jnp.float32)
    for a in range(2):
        for b in range(2):
            for c in range(2):
                total = total + jnp.pad(cells[a, b, c], ((a, 1 - a), (b, 1 - b), (c, 1 - c)))
    return total


def lor_diagonal(coeff, spacing):
    width_x = spacing[0][:, None, None]
    width_y = spacing[1][None, :, None]
    width_z = spacing[2][None, None, :]
    cells = coeff * (
        width_y * width_z / (9.0 * width_x)
        + width_x * width_z / (9.0 * width_y)
        + width_x * width_y / (9.0 * width_z)
    )
    shape = tuple((n + 1 for n in coeff.shape))
    total = jnp.zeros(shape, jnp.float32)
    for a in range(2):
        for b in range(2):
            for c in range(2):
                total = total + jnp.pad(cells, ((a, 1 - a), (b, 1 - b), (c, 1 - c)))
    return total


def subcell_coefficient(kappa):
    averaged = 0.5 * (kappa[:-1] + kappa[1:])
    averaged = 0.5 * (averaged[:, :-1] + averaged[:, 1:])
    averaged = 0.5 * (averaged[:, :, :-1] + averaged[:, :, 1:])
    count_x, count_y, count_z = averaged.shape[3:]
    return jnp.transpose(averaged, (3, 0, 4, 1, 5, 2)).reshape(
        4 * count_x, 4 * count_y, 4 * count_z
    )


def coarsen(coeff):
    nx, ny, nz = coeff.shape
    return jnp.mean(coeff.reshape(nx // 2, 2, ny // 2, 2, nz // 2, 2), axis=(1, 3, 5))


def interp_weights(width):
    paired = width.reshape(-1, 2)
    span = paired[:, 0] + paired[:, 1]
    return (paired[:, 1] / span, paired[:, 0] / span)


def prolong_first(coarse, left, right):
    shape = (-1,) + (1,) * (coarse.ndim - 1)
    middle = left.reshape(shape) * coarse[:-1] + right.reshape(shape) * coarse[1:]
    woven = jnp.stack([coarse[:-1], middle], axis=1).reshape(
        (2 * (coarse.shape[0] - 1),) + coarse.shape[1:]
    )
    return jnp.concatenate([woven, coarse[-1:]], axis=0)


def restrict_first(fine, left, right):
    shape = (-1,) + (1,) * (fine.ndim - 1)
    middle = fine[1::2]
    spare = [(0, 0)] * (fine.ndim - 1)
    return (
        fine[0::2]
        + jnp.pad(left.reshape(shape) * middle, [(0, 1)] + spare)
        + jnp.pad(right.reshape(shape) * middle, [(1, 0)] + spare)
    )


def prolong(coarse, weight_sets):
    for axis in range(3):
        left, right = weight_sets[axis]
        coarse = jnp.moveaxis(prolong_first(jnp.moveaxis(coarse, axis, 0), left, right), 0, axis)
    return coarse


def restrict(fine, weight_sets):
    for axis in range(3):
        left, right = weight_sets[axis]
        fine = jnp.moveaxis(restrict_first(jnp.moveaxis(fine, axis, 0), left, right), 0, axis)
    return fine


def collapse_leading(padded):
    inner = padded[1:-1]
    head = inner[0] + padded[0]
    tail = inner[-1] + padded[-1]
    return jnp.concatenate([head[None], inner[1:-1], tail[None]], axis=0)


def fold_axis(padded, axis):
    return jnp.moveaxis(collapse_leading(jnp.moveaxis(padded, axis, 0)), 0, axis)


def assemble(partial_value):
    padded = extended(partial_value, (("gx", 0), ("gy", 1), ("gz", 2)), 1)
    return fold_axis(fold_axis(fold_axis(padded, 0), 1), 2)


def side_mask(cells, position, devices):
    index = position * cells + jnp.arange(cells + 1)
    return ((index > 0) & (index < cells * devices)).astype(jnp.float32)


def block_mask(shape):
    mask_x = side_mask(shape[0], lax.axis_index("gx"), lax.axis_size("gx"))
    mask_y = side_mask(shape[1], lax.axis_index("gy"), lax.axis_size("gy"))
    mask_z = side_mask(shape[2], lax.axis_index("gz"), lax.axis_size("gz"))
    return mask_x[:, None, None] * mask_y[None, :, None] * mask_z[None, None, :]


def owned_mask(shape):
    sides = [(jnp.arange(n + 1) >= 1).astype(jnp.float32) for n in shape]
    return sides[0][:, None, None] * sides[1][None, :, None] * sides[2][None, None, :]


def cycle(level, forcing, levels):
    coeff, spacing, diag, mask, weight_sets, owned = levels[level]
    guess = relax_weight * forcing / diag
    if level == LEVELS - 1:
        guess = (
            guess
            + relax_weight * (forcing - mask * assemble(lor_terms(guess, coeff, spacing))) / diag
        )
        return guess
    defect = forcing * owned - lor_terms(guess, coeff, spacing)
    coarse = levels[level + 1][3] * assemble(restrict(defect, weight_sets))
    guess = guess + prolong(cycle(level + 1, coarse, levels), weight_sets)
    return (
        guess + relax_weight * (forcing - mask * assemble(lor_terms(guess, coeff, spacing))) / diag
    )


def inner_pair(resid, precond, image):
    local_rho = jnp.sum(resid[1:, 1:, 1:] * precond[1:, 1:, 1:])
    local_curv = jnp.sum(precond[1:, 1:, 1:] * image[1:, 1:, 1:])
    return lax.psum((local_rho, local_curv), ("gx", "gy", "gz"))


def body(kappa, source):
    points, quad_weights, deriv = gll_tables()
    cube = (
        quad_weights[:, None, None] * quad_weights[None, :, None] * quad_weights[None, None, :]
    ).reshape(5, 5, 5, 1, 1, 1)
    weighted = kappa * cube
    counts = kappa.shape[3:]
    finest_mask = block_mask([4 * c for c in counts])
    rhs = finest_mask * assemble(node_sum(cube * source))
    gaps = points[1:] - points[:-1]
    spacing = [jnp.tile(gaps, c) for c in counts]
    coeff = subcell_coefficient(kappa)
    levels = []
    for level in range(LEVELS):
        weight_sets = [interp_weights(h) for h in spacing] if level < LEVELS - 1 else None
        diag = assemble(lor_diagonal(coeff, spacing))
        levels.append(
            (coeff, spacing, diag, block_mask(coeff.shape), weight_sets, owned_mask(coeff.shape))
        )
        if level < LEVELS - 1:
            coeff = coarsen(coeff)
            spacing = [h.reshape(-1, 2).sum(axis=1) for h in spacing]

    def operator(field):
        return finest_mask * assemble(stiffness_terms(field, weighted, deriv))

    resid = rhs
    precond = cycle(0, resid, levels)
    image = operator(precond)
    rho_old, curv = inner_pair(resid, precond, image)
    alpha = rho_old / curv
    direction, along = (precond, image)
    iterate = alpha * direction
    resid = resid - alpha * along
    precond = cycle(0, resid, levels)
    image = operator(precond)
    rho_new, curv = inner_pair(resid, precond, image)
    ratio = rho_new / rho_old
    alpha = rho_new / (curv - ratio * rho_new / alpha)
    direction = precond + ratio * direction
    along = image + ratio * along
    iterate = iterate + alpha * direction
    resid = resid - alpha * along
    return (iterate[1:, 1:, 1:], resid[1:, 1:, 1:])


def exact_tables():
    points = np.array([-1.0, -math.sqrt(3.0 / 7.0), 0.0, math.sqrt(3.0 / 7.0), 1.0])
    quad_weights = np.array([0.1, 49.0 / 90.0, 32.0 / 45.0, 49.0 / 90.0, 0.1])
    bary = np.array(
        [np.prod([points[i] - points[k] for k in range(5) if k != i]) for i in range(5)]
    )
    deriv = np.zeros((5, 5))
    for i in range(5):
        for j in range(5):
            if i != j:
                deriv[i, j] = bary[i] / (bary[j] * (points[i] - points[j]))
    for i in range(5):
        deriv[i, i] = -np.sum(deriv[i])
    return points, quad_weights, deriv


def level_widths():
    points = exact_tables()[0]
    widths = [[float(h) for h in points[1:] - points[:-1]]]
    for _ in range(LEVELS - 1):
        last = widths[-1]
        widths.append([last[2 * i] + last[2 * i + 1] for i in range(len(last) // 2)])
    return widths


def cell_scales(hx, hy, hz):
    mass = lambda h, odd: h / 12.0 if odd else h / 4.0
    scales = {}
    for p in range(2):
        for q in range(2):
            for r in range(2):
                scale = 0.0
                if p:
                    scale += mass(hy, q) * mass(hz, r) / hx
                if q:
                    scale += mass(hx, p) * mass(hz, r) / hy
                if r:
                    scale += mass(hx, p) * mass(hy, q) / hz
                scales[p, q, r] = scale
    return scales


def iteration_kernel(near, far, x_out, r_out, weighted, full, part, c0, c1, c2,
                     d0, d1, d2, f1, f2, g1, p1, g2, p2, resid, precond, direction,
                     iterate, gathered, arrivals, *, ny, offsets):
    rows, lanes = resid.shape[1:]
    at_x, at_y, at_z = (lax.axis_index(axis) for axis in ("gx", "gy", "gz"))
    flat = (at_x * ny + at_y) * 2 + at_z
    span = near.shape[1]
    copies = []
    for side, (ref, base) in enumerate(((near, 0), (far, 2 * ny))):
        for i, offset in enumerate(offsets):
            copies.append(pltpu.make_async_copy(
                ref.at[i],
                gathered.at[pl.ds((flat ^ (offset ^ base)) * span, span)],
                arrivals.at[side * len(offsets) + i],
            ))
    for copy in copies:
        copy.start()
    stride = gathered.shape[0] // rows
    half = stride // 2
    points, quad, deriv = exact_tables()
    widths = level_widths()
    cells = [len(h) for h in widths]
    coeffs, diags = (c0, c1, c2), (d0, d1, d2)
    fulls, parts = (full, g1, g2), (part, p1, p2)

    sub = lax.broadcasted_iota(jnp.int32, (rows, lanes), 0)
    lane = lax.broadcasted_iota(jnp.int32, (rows, lanes), 1)
    masks = (
        (sub < rows - ny).astype(jnp.float32),
        (sub % ny < ny - 1).astype(jnp.float32),
        (lane < lanes - 1).astype(jnp.float32),
    )

    def before(tile, dim):
        if dim == 2:
            return pltpu.roll(tile, 1, 1)
        return pltpu.roll(tile, (ny, 1)[dim], 0)

    def after(tile, dim):
        if dim == 2:
            return pltpu.roll(tile, lanes - 1, 1)
        return pltpu.roll(tile, rows - (ny, 1)[dim], 0)

    def at(n, a, b, c):
        return (a * (n + 1) + b) * (n + 1) + c

    def own(n, a, b, c):
        return ((a - 1) * n + b - 1) * n + c - 1

    def inside(n, a, b, c, tile):
        for dim, offset in enumerate((a, b, c)):
            if offset == n:
                tile = tile * masks[dim]
        return tile

    def ghosts(ref, n):
        for a in range(1, n + 1):
            for b in range(1, n + 1):
                ref[at(n, a, b, 0)] = before(ref[at(n, a, b, n)], 2)
            for c in range(n + 1):
                ref[at(n, a, 0, c)] = before(ref[at(n, a, n, c)], 1)
        for b in range(n + 1):
            for c in range(n + 1):
                ref[at(n, 0, b, c)] = before(ref[at(n, n, b, c)], 0)

    def fold(ref, n):
        for a in range(n + 1):
            for b in range(n + 1):
                ref[at(n, a, b, n)] += after(ref[at(n, a, b, 0)], 2)
            for c in range(1, n + 1):
                ref[at(n, a, n, c)] += after(ref[at(n, a, 0, c)], 1)
        for b in range(1, n + 1):
            for c in range(1, n + 1):
                ref[at(n, n, b, c)] += after(ref[at(n, 0, b, c)], 0)

    def owned(n):
        for a in range(1, n + 1):
            for b in range(1, n + 1):
                for c in range(1, n + 1):
                    yield a, b, c

    def lor(level):
        n, h = cells[level], widths[level]
        src, dst, coeff = fulls[level], parts[level], coeffs[level]
        ghosts(src, n)
        for b in range(n):
            for c in range(n):
                carried = None
                face = None
                for a in range(n + 1):
                    u = [[src[at(n, a, b + i, c + k)] for k in range(2)] for i in range(2)]
                    sums = [u[i][1] + u[i][0] for i in range(2)]
                    difs = [u[i][1] - u[i][0] for i in range(2)]
                    now = {
                        (0, 0): sums[1] + sums[0],
                        (1, 0): sums[1] - sums[0],
                        (0, 1): difs[1] + difs[0],
                        (1, 1): difs[1] - difs[0],
                    }
                    lower = {}
                    upper = {}
                    if a > 0:
                        scales = cell_scales(h[a - 1], h[b], h[c])
                        k = coeff[own(n, a, b + 1, c + 1)]
                        for key in now:
                            odd = ((now[key] - face[key]) * scales[(1,) + key]) * k
                            if key == (0, 0):
                                lower[key], upper[key] = -odd, odd
                            else:
                                even = ((now[key] + face[key]) * scales[(0,) + key]) * k
                                lower[key], upper[key] = even - odd, even + odd
                        total = {
                            key: lower[key] if carried is None else lower[key] + carried[key]
                            for key in now
                        }
                        spread(dst, n, a - 1, b, c, total)
                    face = now
                    carried = upper if a > 0 else None
                spread(dst, n, n, b, c, carried)
        fold(dst, n)

    def spread(dst, n, a, b, c, total):
        s1 = total[0, 0] + total[1, 0]
        s0 = total[0, 0] - total[1, 0]
        d1_ = total[0, 1] + total[1, 1]
        d0_ = total[0, 1] - total[1, 1]
        for i, s, d in ((0, s0, d0_), (1, s1, d1_)):
            for k, value in ((0, s - d), (1, s + d)):
                spot = at(n, a, b + i, c + k)
                if (i == 1 or b == 0) and (k == 1 or c == 0):
                    dst[spot] = value
                else:
                    dst[spot] += value

    def diagonal(level):
        n, h = cells[level], widths[level]
        dst, coeff = parts[level], coeffs[level]
        tiles = {}
        for a in range(n):
            for b in range(n):
                for c in range(n):
                    hx, hy, hz = h[a], h[b], h[c]
                    scale = hy * hz / (9 * hx) + hx * hz / (9 * hy) + hx * hy / (9 * hz)
                    tile = coeff[own(n, a + 1, b + 1, c + 1)] * scale
                    for i in range(2):
                        for j in range(2):
                            for k in range(2):
                                spot = at(n, a + i, b + j, c + k)
                                first = (i or a == 0) and (j or b == 0) and (k or c == 0)
                                if first:
                                    dst[spot] = tile
                                else:
                                    dst[spot] += tile
        fold(dst, n)
        for a, b, c in owned(n):
            diags[level][own(n, a, b, c)] = relax_weight / dst[at(n, a, b, c)]

    def pair_weights(level):
        h = widths[level]
        spans = [(h[2 * i], h[2 * i + 1]) for i in range(len(h) // 2)]
        return [q / (p + q) for p, q in spans], [p / (p + q) for p, q in spans]

    def restrict_to(level, defect, target):
        n = cells[level]
        m = n // 2
        left, right = pair_weights(level)

        def line(values, dim):
            result = []
            for o in range(1, m + 1):
                beyond = values[2 * o] if o < m else after(values[0], dim)
                result.append(
                    values[2 * o - 1] + right[o - 1] * values[2 * o - 2] + left[o % m] * beyond
                )
            return result

        slabs = []
        for a in range(1, n + 1):
            lines = [line([defect(a, b, c) for c in range(1, n + 1)], 2) for b in range(1, n + 1)]
            turned = [line([lines[b][c] for b in range(n)], 1) for c in range(m)]
            slabs.append(turned)
        for c in range(m):
            for b in range(m):
                out = line([slabs[a][c][b] for a in range(n)], 0)
                for a in range(m):
                    target[own(m, a + 1, b + 1, c + 1)] = inside(m, a + 1, b + 1, c + 1, out[a])

    def prolong_from(level, add):
        n = cells[level]
        m = n // 2
        left, right = pair_weights(level)
        src = fulls[level + 1]
        ghosts(src, m)

        def line(values):
            result = []
            for o in range(1, m + 1):
                result.append(left[o - 1] * values[o - 1] + right[o - 1] * values[o])
                result.append(values[o])
            return result

        slabs = []
        for a in range(m + 1):
            lines = [line([src[at(m, a, b, c)] for c in range(m + 1)]) for b in range(m + 1)]
            slabs.append([line([lines[b][c] for b in range(m + 1)]) for c in range(n)])
        for c in range(n):
            for b in range(n):
                out = line([slabs[a][c][b] for a in range(m + 1)])
                for a in range(n):
                    add(a + 1, b + 1, c + 1, out[a])

    def cycle_at(level, forcing, store):
        n = cells[level]
        src, dst, diag = fulls[level], parts[level], diags[level]
        for a, b, c in owned(n):
            spot = own(n, a, b, c)
            src[at(n, a, b, c)] = forcing[spot] * diag[spot]
        lor(level)
        if level < LEVELS - 1:
            restrict_to(
                level,
                lambda a, b, c: forcing[own(n, a, b, c)] - dst[at(n, a, b, c)],
                (f1, f2)[level],
            )

            def leave(a, b, c, tile):
                fulls[level + 1][at(n // 2, a, b, c)] = tile

            cycle_at(level + 1, (f1, f2)[level], leave)

            def add(a, b, c, tile):
                src[at(n, a, b, c)] += tile

            prolong_from(level, add)
            lor(level)
        for a, b, c in owned(n):
            spot = own(n, a, b, c)
            change = inside(n, a, b, c, (forcing[spot] - dst[at(n, a, b, c)]) * diag[spot])
            store(a, b, c, src[at(n, a, b, c)] + change)

    def derive(u):
        e = [u[0] + u[4], u[1] + u[3], u[2]]
        o = [u[0] - u[4], u[1] - u[3]]
        odd = []
        even = []
        for i in range(2):
            odd.append(sum(
                e[j] * float((deriv[i, j] + deriv[i, 4 - j]) / 2 if j < 2 else deriv[i, 2])
                for j in range(3)
            ))
        for i in range(3):
            even.append(sum(o[j] * float((deriv[i, j] - deriv[i, 4 - j]) / 2) for j in range(2)))
        return [even[0] + odd[0], even[1] + odd[1], even[2], even[1] - odd[1], even[0] - odd[0]]

    def derive_back(g):
        e = [g[0] + g[4], g[1] + g[3], g[2]]
        o = [g[0] - g[4], g[1] - g[3]]
        odd = []
        even = []
        for a in range(2):
            odd.append(sum(
                e[j] * float((deriv[j, a] + deriv[4 - j, a]) / 2 if j < 2 else deriv[2, a])
                for j in range(3)
            ))
        for a in range(3):
            even.append(sum(o[j] * float((deriv[j, a] - deriv[4 - j, a]) / 2) for j in range(2)))
        return [even[0] + odd[0], even[1] + odd[1], even[2], even[1] - odd[1], even[0] - odd[0]]

    def stiffness():
        ghosts(full, 4)

        def run(spots, first):
            grad = derive([full[s] for s in spots])
            back = derive_back([grad[i] * weighted[s] for i, s in enumerate(spots)])
            for s, value in zip(spots, back):
                if first:
                    part[s] = value
                else:
                    part[s] += value

        def outer(i, carry):
            for k in range(5):
                run([25 * i + 5 * k + t for t in range(5)], True)
            for k in range(5):
                run([25 * i + 5 * t + k for t in range(5)], False)
            return carry

        def along(i, carry):
            for k in range(5):
                run([25 * t + 5 * i + k for t in range(5)], False)
            return carry

        lax.fori_loop(0, 5, outer, 0)
        lax.fori_loop(0, 5, along, 0)
        fold(part, 4)

    for copy in copies:
        copy.wait()

    low = lane < lanes // 2
    for a in range(5):
        for b in range(5):
            for c in range(5):
                spot = 25 * a + 5 * b + c
                first = gathered[pl.ds(spot, rows, stride=stride), :]
                second = gathered[pl.ds(half + spot, rows, stride=stride), :]
                cube = float(quad[a] * quad[b] * quad[c])
                full[spot] = jnp.where(low, first, pltpu.roll(second, lanes // 2, 1))
                part[spot] = jnp.where(low, pltpu.roll(first, lanes // 2, 1), second) * cube
                weighted[spot] = full[spot] * cube
    fold(part, 4)
    for a, b, c in owned(4):
        resid[own(4, a, b, c)] = inside(4, a, b, c, part[at(4, a, b, c)])
    for a in range(4):
        for b in range(4):
            plane = [
                (full[at(4, a, b, c)] + full[at(4, a + 1, b, c)])
                + (full[at(4, a, b + 1, c)] + full[at(4, a + 1, b + 1, c)])
                for c in range(5)
            ]
            for c in range(4):
                c0[own(4, a + 1, b + 1, c + 1)] = (plane[c] + plane[c + 1]) * 0.125
    for level in range(LEVELS - 1):
        m = cells[level + 1]
        for a, b, c in owned(m):
            total = None
            for i in range(2):
                for j in range(2):
                    for k in range(2):
                        tile = coeffs[level][
                            own(2 * m, 2 * a - i, 2 * b - j, 2 * c - k)
                        ]
                        total = tile if total is None else total + tile
            coeffs[level + 1][own(m, a, b, c)] = total * 0.125
    for level in range(LEVELS):
        diagonal(level)

    direction[...] = jnp.zeros_like(direction)
    iterate[...] = jnp.zeros_like(iterate)

    def settle(a, b, c, tile):
        precond[own(4, a, b, c)] = tile

    def product(tiles):
        total = None
        for tile in tiles:
            total = tile if total is None else total + tile
        return jnp.sum(jnp.sum(total, axis=0, keepdims=True), axis=1, keepdims=True)

    def step(number, rho_old):
        cycle_at(0, resid, settle)
        rho = product(resid[i] * precond[i] for i in range(64))
        ratio = jnp.where(number == 0, 0.0, rho / rho_old)
        for a, b, c in owned(4):
            spot = own(4, a, b, c)
            value = precond[spot] + ratio * direction[spot]
            direction[spot] = value
            full[at(4, a, b, c)] = value
        stiffness()
        curv = None
        for a, b, c in owned(4):
            image = inside(4, a, b, c, part[at(4, a, b, c)])
            precond[own(4, a, b, c)] = image
            term = direction[own(4, a, b, c)] * image
            curv = term if curv is None else curv + term
        alpha = rho / product([curv])
        for i in range(64):
            iterate[i] += alpha * direction[i]
            resid[i] -= alpha * precond[i]
        return rho

    lax.fori_loop(0, 2, step, jnp.ones((1, 1), jnp.float32))

    row = at_x * ny + at_y
    start = at_z * (lanes // 2)
    width = x_out.shape[2]
    ez = lax.broadcasted_iota(jnp.int32, (lanes, width), 0)
    spot_z = lax.broadcasted_iota(jnp.int32, (lanes, width), 1)
    for out, ref in ((x_out, iterate), (r_out, resid)):
        total = jnp.zeros((16, width), jnp.float32)
        for c in range(4):
            pick = (spot_z == 4 * (ez - start) + c).astype(jnp.float32)
            lines = jnp.concatenate(
                [ref[4 * ab + c, pl.ds(row, 1), :] for ab in range(16)], axis=0
            )
            total = total + jnp.dot(
                lines, pick, precision=lax.Precision.HIGHEST,
                preferred_element_type=jnp.float32,
            )
        for a in range(4):
            out[a] = total[4 * a : 4 * a + 4]


def exchange_offsets(nx, ny):
    strips = [2 * d for d in (0, 1, 3, 2)[:ny]] if ny <= 4 else [2 * d for d in range(ny)]
    return [
        (strip, across)
        for strip in strips
        for across in [4 * ny * i + z for z in range(2) for i in range(nx // 2)]
    ]


def whole_body(kappa, source):
    axes = ("gx", "gy", "gz")
    nx, ny = lax.axis_size("gx"), lax.axis_size("gy")
    rows, lanes = nx * ny, 2 * kappa.shape[5]

    def swap(block, distance):
        return lax.ppermute(block, axes, [(i, i ^ distance) for i in range(2 * rows)])

    packed = jnp.concatenate([kappa.reshape(125, -1), source.reshape(125, -1)], axis=1)
    packed = jnp.pad(packed, ((0, 3), (0, 0)))
    offsets = exchange_offsets(nx, ny)
    strips = {}
    pieces = []
    for strip, across in offsets:
        if across == 0:
            strips[strip] = swap(packed, strip) if strip else packed
            pieces.append(strips[strip])
        else:
            pieces.append(swap(strips[strip], across))
    near = jnp.stack(pieces)
    far = swap(near, 2 * ny)

    def tiles(count):
        return pltpu.VMEM((count, rows, lanes), jnp.float32)

    counts = [125, 125, 125, 64, 8, 1, 64, 8, 1, 8, 1, 27, 27, 8, 8, 64, 64, 64, 64]
    shape = jax.ShapeDtypeStruct((4, 4, 2 * lanes), jnp.float32)
    vmem = pl.BlockSpec(memory_space=pltpu.VMEM)
    anywhere = pl.BlockSpec(memory_space=pl.ANY)
    return tuple(pl.pallas_call(
        lambda *refs: iteration_kernel(
            *refs, ny=ny, offsets=[strip ^ across for strip, across in offsets]
        ),
        out_shape=(shape, shape),
        in_specs=[anywhere, anywhere],
        out_specs=(vmem, vmem),
        scratch_shapes=[tiles(n) for n in counts]
        + [pltpu.VMEM((2 * rows * 128, lanes), jnp.float32)]
        + [pltpu.SemaphoreType.DMA((2 * len(offsets),))],
        compiler_params=pltpu.CompilerParams(vmem_limit_bytes=40 * 2**20),
        name="whole_iteration",
    )(near, far))


def fits_whole(kappa, mesh):
    sizes = mesh.shape
    rows = sizes["gx"] * sizes["gy"]
    one_column = kappa.shape[3] == sizes["gx"] and kappa.shape[4] == sizes["gy"]
    lanes = kappa.shape[5]
    return (
        one_column
        and sizes["gz"] == 2
        and all(n & (n - 1) == 0 and n > 1 for n in (sizes["gx"], sizes["gy"]))
        and rows % 8 == 0
        and lanes % 128 == 0
        and rows * lanes <= 16 * 128
    )


def solution(mesh):
    placed = (P(None, None, None, "gx", "gy", "gz"), P(None, None, None, "gx", "gy", "gz"))

    def run(kappa, source):
        return jax.shard_map(
            whole_body if fits_whole(kappa, mesh) else body,
            mesh=mesh,
            in_specs=placed,
            out_specs=(P("gx", "gy", "gz"), P("gx", "gy", "gz")),
            check_vma=False,
        )(kappa, source)

    return run
```

```python
import math

import jax
import jax.numpy as jnp
import numpy as np
from jax import lax
from jax.experimental import pallas as pl
from jax.experimental.pallas import tpu as pltpu
from jax.sharding import PartitionSpec as P

LEVELS = 3


relax_weight = 0.6


def extended(cells, sides, width):
    for axis, dim in sides:
        count = lax.axis_size(axis)
        ends = count - 1
        head = lax.slice_in_dim(cells, 0, width, axis=dim)
        tail = lax.slice_in_dim(cells, cells.shape[dim] - width, cells.shape[dim], axis=dim)
        cells = jnp.concatenate(
            [
                lax.ppermute(tail, axis, [(i, (i + 1) % count) for i in range(ends)]),
                cells,
                lax.ppermute(head, axis, [((i + 1) % count, i) for i in range(ends)]),
            ],
            axis=dim,
        )
    return cells


def gll_tables():
    points = np.array([-1.0, -math.sqrt(3.0 / 7.0), 0.0, math.sqrt(3.0 / 7.0), 1.0])
    quad_weights = np.array([0.1, 49.0 / 90.0, 32.0 / 45.0, 49.0 / 90.0, 0.1])
    bary = np.array(
        [np.prod([points[i] - points[k] for k in range(5) if k != i]) for i in range(5)]
    )
    deriv = np.zeros((5, 5))
    for i in range(5):
        for j in range(5):
            if i != j:
                deriv[i, j] = bary[i] / (bary[j] * (points[i] - points[j]))
    for i in range(5):
        deriv[i, i] = -np.sum(deriv[i])
    return (
        jnp.asarray(points, jnp.float32),
        jnp.asarray(quad_weights, jnp.float32),
        jnp.asarray(deriv, jnp.float32),
    )


def split_first(values):
    count = (values.shape[0] - 1) // 4
    lower = jnp.swapaxes(values[:-1].reshape((count, 4) + values.shape[1:]), 0, 1)
    return jnp.concatenate([lower, values[4::4][None]], axis=0)


def merge_first(block):
    count = block.shape[1]
    rest = block.shape[2:]
    lower = jnp.swapaxes(block[:4], 0, 1).reshape((4 * count,) + rest)
    tail = jnp.concatenate([jnp.zeros((count, 3) + rest, block.dtype), block[4][:, None]], axis=1)
    tail = tail.reshape((4 * count,) + rest)
    spare = [(0, 0)] * len(rest)
    return jnp.pad(lower, [(0, 1)] + spare) + jnp.pad(tail, [(1, 0)] + spare)


def element_view(field):
    element_portion = split_first(field)
    element_portion = split_first(jnp.moveaxis(element_portion, 2, 0))
    element_portion = split_first(jnp.moveaxis(element_portion, 4, 0))
    return jnp.transpose(element_portion, (4, 2, 0, 5, 3, 1))


def node_sum(block):
    element_portion = jnp.transpose(block, (2, 5, 1, 4, 0, 3))
    element_portion = jnp.moveaxis(merge_first(element_portion), 0, 4)
    element_portion = jnp.moveaxis(merge_first(element_portion), 0, 2)
    return merge_first(element_portion)


def stiffness_terms(field, weighted, deriv):
    highest = lax.Precision.HIGHEST
    local = element_view(field)
    grad_x = jnp.einsum("ia,abcxyz->ibcxyz", deriv, local, precision=highest)
    grad_y = jnp.einsum("jb,abcxyz->ajcxyz", deriv, local, precision=highest)
    grad_z = jnp.einsum("kc,abcxyz->abkxyz", deriv, local, precision=highest)
    back = jnp.einsum("ia,ibcxyz->abcxyz", deriv, weighted * grad_x, precision=highest)
    back = back + jnp.einsum("jb,ajcxyz->abcxyz", deriv, weighted * grad_y, precision=highest)
    back = back + jnp.einsum("kc,abkxyz->abcxyz", deriv, weighted * grad_z, precision=highest)
    return node_sum(back)


def mass_pair(paired, width):
    return jnp.stack(
        [width / 6.0 * (2.0 * paired[0] + paired[1]), width / 6.0 * (paired[0] + 2.0 * paired[1])]
    )


def stiff_pair(paired, width):
    slope = (paired[0] - paired[1]) / width
    return jnp.stack([slope, -slope])


def lor_terms(field, coeff, spacing):
    width_x, width_y, width_z = spacing
    zpairs = jnp.stack([field[:, :, :-1], field[:, :, 1:]])
    zmass = mass_pair(zpairs, width_z)
    stiffness_along_z = stiff_pair(zpairs, width_z)
    ymass = jnp.stack([zmass[:, :, :-1], zmass[:, :, 1:]])
    ystiff = jnp.stack([stiffness_along_z[:, :, :-1], stiffness_along_z[:, :, 1:]])
    column_y = width_y[:, None]
    first = mass_pair(ymass, column_y)
    second = stiff_pair(ymass, column_y) + mass_pair(ystiff, column_y)
    column_x = width_x[:, None, None]
    xfirst = jnp.stack([first[:, :, :-1], first[:, :, 1:]])
    xsecond = jnp.stack([second[:, :, :-1], second[:, :, 1:]])
    cells = (stiff_pair(xfirst, column_x) + mass_pair(xsecond, column_x)) * coeff
    total = jnp.zeros(field.shape, jnp.float32)
    for a in range(2):
        for b in range(2):
            for c in range(2):
                total = total + jnp.pad(cells[a, b, c], ((a, 1 - a), (b, 1 - b), (c, 1 - c)))
    return total


def lor_diagonal(coeff, spacing):
    width_x = spacing[0][:, None, None]
    width_y = spacing[1][None, :, None]
    width_z = spacing[2][None, None, :]
    cells = coeff * (
        width_y * width_z / (9.0 * width_x)
        + width_x * width_z / (9.0 * width_y)
        + width_x * width_y / (9.0 * width_z)
    )
    shape = tuple((n + 1 for n in coeff.shape))
    total = jnp.zeros(shape, jnp.float32)
    for a in range(2):
        for b in range(2):
            for c in range(2):
                total = total + jnp.pad(cells, ((a, 1 - a), (b, 1 - b), (c, 1 - c)))
    return total


def subcell_coefficient(kappa):
    averaged = 0.5 * (kappa[:-1] + kappa[1:])
    averaged = 0.5 * (averaged[:, :-1] + averaged[:, 1:])
    averaged = 0.5 * (averaged[:, :, :-1] + averaged[:, :, 1:])
    count_x, count_y, count_z = averaged.shape[3:]
    return jnp.transpose(averaged, (3, 0, 4, 1, 5, 2)).reshape(
        4 * count_x, 4 * count_y, 4 * count_z
    )


def coarsen(coeff):
    nx, ny, nz = coeff.shape
    return jnp.mean(coeff.reshape(nx // 2, 2, ny // 2, 2, nz // 2, 2), axis=(1, 3, 5))


def interp_weights(width):
    paired = width.reshape(-1, 2)
    span = paired[:, 0] + paired[:, 1]
    return (paired[:, 1] / span, paired[:, 0] / span)


def prolong_first(coarse, left, right):
    shape = (-1,) + (1,) * (coarse.ndim - 1)
    middle = left.reshape(shape) * coarse[:-1] + right.reshape(shape) * coarse[1:]
    woven = jnp.stack([coarse[:-1], middle], axis=1).reshape(
        (2 * (coarse.shape[0] - 1),) + coarse.shape[1:]
    )
    return jnp.concatenate([woven, coarse[-1:]], axis=0)


def restrict_first(fine, left, right):
    shape = (-1,) + (1,) * (fine.ndim - 1)
    middle = fine[1::2]
    spare = [(0, 0)] * (fine.ndim - 1)
    return (
        fine[0::2]
        + jnp.pad(left.reshape(shape) * middle, [(0, 1)] + spare)
        + jnp.pad(right.reshape(shape) * middle, [(1, 0)] + spare)
    )


def prolong(coarse, weight_sets):
    for axis in range(3):
        left, right = weight_sets[axis]
        coarse = jnp.moveaxis(prolong_first(jnp.moveaxis(coarse, axis, 0), left, right), 0, axis)
    return coarse


def restrict(fine, weight_sets):
    for axis in range(3):
        left, right = weight_sets[axis]
        fine = jnp.moveaxis(restrict_first(jnp.moveaxis(fine, axis, 0), left, right), 0, axis)
    return fine


def collapse_leading(padded):
    inner = padded[1:-1]
    head = inner[0] + padded[0]
    tail = inner[-1] + padded[-1]
    return jnp.concatenate([head[None], inner[1:-1], tail[None]], axis=0)


def fold_axis(padded, axis):
    return jnp.moveaxis(collapse_leading(jnp.moveaxis(padded, axis, 0)), 0, axis)


def assemble(partial_value):
    padded = extended(partial_value, (("gx", 0), ("gy", 1), ("gz", 2)), 1)
    return fold_axis(fold_axis(fold_axis(padded, 0), 1), 2)


def side_mask(cells, position, devices):
    index = position * cells + jnp.arange(cells + 1)
    return ((index > 0) & (index < cells * devices)).astype(jnp.float32)


def block_mask(shape):
    mask_x = side_mask(shape[0], lax.axis_index("gx"), lax.axis_size("gx"))
    mask_y = side_mask(shape[1], lax.axis_index("gy"), lax.axis_size("gy"))
    mask_z = side_mask(shape[2], lax.axis_index("gz"), lax.axis_size("gz"))
    return mask_x[:, None, None] * mask_y[None, :, None] * mask_z[None, None, :]


def owned_mask(shape):
    sides = [(jnp.arange(n + 1) >= 1).astype(jnp.float32) for n in shape]
    return sides[0][:, None, None] * sides[1][None, :, None] * sides[2][None, None, :]


def cycle(level, forcing, levels):
    coeff, spacing, diag, mask, weight_sets, owned = levels[level]
    guess = relax_weight * forcing / diag
    if level == LEVELS - 1:
        guess = (
            guess
            + relax_weight * (forcing - mask * assemble(lor_terms(guess, coeff, spacing))) / diag
        )
        return guess
    defect = forcing * owned - lor_terms(guess, coeff, spacing)
    coarse = levels[level + 1][3] * assemble(restrict(defect, weight_sets))
    guess = guess + prolong(cycle(level + 1, coarse, levels), weight_sets)
    return (
        guess + relax_weight * (forcing - mask * assemble(lor_terms(guess, coeff, spacing))) / diag
    )


def inner_pair(resid, precond, image):
    local_rho = jnp.sum(resid[1:, 1:, 1:] * precond[1:, 1:, 1:])
    local_curv = jnp.sum(precond[1:, 1:, 1:] * image[1:, 1:, 1:])
    return lax.psum((local_rho, local_curv), ("gx", "gy", "gz"))


def body(kappa, source):
    points, quad_weights, deriv = gll_tables()
    cube = (
        quad_weights[:, None, None] * quad_weights[None, :, None] * quad_weights[None, None, :]
    ).reshape(5, 5, 5, 1, 1, 1)
    weighted = kappa * cube
    counts = kappa.shape[3:]
    finest_mask = block_mask([4 * c for c in counts])
    rhs = finest_mask * assemble(node_sum(cube * source))
    gaps = points[1:] - points[:-1]
    spacing = [jnp.tile(gaps, c) for c in counts]
    coeff = subcell_coefficient(kappa)
    levels = []
    for level in range(LEVELS):
        weight_sets = [interp_weights(h) for h in spacing] if level < LEVELS - 1 else None
        diag = assemble(lor_diagonal(coeff, spacing))
        levels.append(
            (coeff, spacing, diag, block_mask(coeff.shape), weight_sets, owned_mask(coeff.shape))
        )
        if level < LEVELS - 1:
            coeff = coarsen(coeff)
            spacing = [h.reshape(-1, 2).sum(axis=1) for h in spacing]

    def operator(field):
        return finest_mask * assemble(stiffness_terms(field, weighted, deriv))

    resid = rhs
    precond = cycle(0, resid, levels)
    image = operator(precond)
    rho_old, curv = inner_pair(resid, precond, image)
    alpha = rho_old / curv
    direction, along = (precond, image)
    iterate = alpha * direction
    resid = resid - alpha * along
    precond = cycle(0, resid, levels)
    image = operator(precond)
    rho_new, curv = inner_pair(resid, precond, image)
    ratio = rho_new / rho_old
    alpha = rho_new / (curv - ratio * rho_new / alpha)
    direction = precond + ratio * direction
    along = image + ratio * along
    iterate = iterate + alpha * direction
    resid = resid - alpha * along
    return (iterate[1:, 1:, 1:], resid[1:, 1:, 1:])


def exact_tables():
    points = np.array([-1.0, -math.sqrt(3.0 / 7.0), 0.0, math.sqrt(3.0 / 7.0), 1.0])
    quad_weights = np.array([0.1, 49.0 / 90.0, 32.0 / 45.0, 49.0 / 90.0, 0.1])
    bary = np.array(
        [np.prod([points[i] - points[k] for k in range(5) if k != i]) for i in range(5)]
    )
    deriv = np.zeros((5, 5))
    for i in range(5):
        for j in range(5):
            if i != j:
                deriv[i, j] = bary[i] / (bary[j] * (points[i] - points[j]))
    for i in range(5):
        deriv[i, i] = -np.sum(deriv[i])
    return points, quad_weights, deriv


def level_widths():
    points = exact_tables()[0]
    widths = [[float(h) for h in points[1:] - points[:-1]]]
    for _ in range(LEVELS - 1):
        last = widths[-1]
        widths.append([last[2 * i] + last[2 * i + 1] for i in range(len(last) // 2)])
    return widths


def cell_scales(hx, hy, hz):
    mass = lambda h, odd: h / 12.0 if odd else h / 4.0
    scales = {}
    for p in range(2):
        for q in range(2):
            for r in range(2):
                scale = 0.0
                if p:
                    scale += mass(hy, q) * mass(hz, r) / hx
                if q:
                    scale += mass(hx, p) * mass(hz, r) / hy
                if r:
                    scale += mass(hx, p) * mass(hy, q) / hz
                scales[p, q, r] = scale
    return scales


def iteration_kernel(near, far, x_out, r_out, weighted, full, part, c0, c1, c2,
                     d0, d1, d2, f1, f2, g1, p1, g2, p2, resid, precond, direction,
                     iterate, gathered, arrivals, *, ny, offsets):
    rows, lanes = resid.shape[1:]
    at_x, at_y, at_z = (lax.axis_index(axis) for axis in ("gx", "gy", "gz"))
    flat = (at_x * ny + at_y) * 2 + at_z
    span = near.shape[1]
    copies = []
    for side, (ref, base) in enumerate(((near, 0), (far, 2 * ny))):
        for i, offset in enumerate(offsets):
            copies.append(pltpu.make_async_copy(
                ref.at[i],
                gathered.at[pl.ds((flat ^ (offset ^ base)) * span, span)],
                arrivals.at[side * len(offsets) + i],
            ))
    for copy in copies:
        copy.start()
    stride = gathered.shape[0] // rows
    half = stride // 2
    points, quad, deriv = exact_tables()
    widths = level_widths()
    cells = [len(h) for h in widths]
    coeffs, diags = (c0, c1, c2), (d0, d1, d2)
    fulls, parts = (full, g1, g2), (part, p1, p2)

    sub = lax.broadcasted_iota(jnp.int32, (rows, lanes), 0)
    lane = lax.broadcasted_iota(jnp.int32, (rows, lanes), 1)
    masks = (
        (sub < rows - ny).astype(jnp.float32),
        (sub % ny < ny - 1).astype(jnp.float32),
        (lane < lanes - 1).astype(jnp.float32),
    )

    def before(tile, dim):
        if dim == 2:
            return pltpu.roll(tile, 1, 1)
        return pltpu.roll(tile, (ny, 1)[dim], 0)

    def after(tile, dim):
        if dim == 2:
            return pltpu.roll(tile, lanes - 1, 1)
        return pltpu.roll(tile, rows - (ny, 1)[dim], 0)

    def at(n, a, b, c):
        return (a * (n + 1) + b) * (n + 1) + c

    def own(n, a, b, c):
        return ((a - 1) * n + b - 1) * n + c - 1

    def inside(n, a, b, c, tile):
        for dim, offset in enumerate((a, b, c)):
            if offset == n:
                tile = tile * masks[dim]
        return tile

    def ghosts(ref, n):
        for a in range(1, n + 1):
            for b in range(1, n + 1):
                ref[at(n, a, b, 0)] = before(ref[at(n, a, b, n)], 2)
            for c in range(n + 1):
                ref[at(n, a, 0, c)] = before(ref[at(n, a, n, c)], 1)
        for b in range(n + 1):
            for c in range(n + 1):
                ref[at(n, 0, b, c)] = before(ref[at(n, n, b, c)], 0)

    def fold(ref, n):
        for a in range(n + 1):
            for b in range(n + 1):
                ref[at(n, a, b, n)] += after(ref[at(n, a, b, 0)], 2)
            for c in range(1, n + 1):
                ref[at(n, a, n, c)] += after(ref[at(n, a, 0, c)], 1)
        for b in range(1, n + 1):
            for c in range(1, n + 1):
                ref[at(n, n, b, c)] += after(ref[at(n, 0, b, c)], 0)

    def owned(n):
        for a in range(1, n + 1):
            for b in range(1, n + 1):
                for c in range(1, n + 1):
                    yield a, b, c

    def lor(level):
        n, h = cells[level], widths[level]
        src, dst, coeff = fulls[level], parts[level], coeffs[level]
        ghosts(src, n)
        for b in range(n):
            for c in range(n):
                carried = None
                face = None
                for a in range(n + 1):
                    u = [[src[at(n, a, b + i, c + k)] for k in range(2)] for i in range(2)]
                    sums = [u[i][1] + u[i][0] for i in range(2)]
                    difs = [u[i][1] - u[i][0] for i in range(2)]
                    now = {
                        (0, 0): sums[1] + sums[0],
                        (1, 0): sums[1] - sums[0],
                        (0, 1): difs[1] + difs[0],
                        (1, 1): difs[1] - difs[0],
                    }
                    lower = {}
                    upper = {}
                    if a > 0:
                        scales = cell_scales(h[a - 1], h[b], h[c])
                        k = coeff[own(n, a, b + 1, c + 1)]
                        for key in now:
                            odd = ((now[key] - face[key]) * scales[(1,) + key]) * k
                            if key == (0, 0):
                                lower[key], upper[key] = -odd, odd
                            else:
                                even = ((now[key] + face[key]) * scales[(0,) + key]) * k
                                lower[key], upper[key] = even - odd, even + odd
                        total = {
                            key: lower[key] if carried is None else lower[key] + carried[key]
                            for key in now
                        }
                        spread(dst, n, a - 1, b, c, total)
                    face = now
                    carried = upper if a > 0 else None
                spread(dst, n, n, b, c, carried)
        fold(dst, n)

    def spread(dst, n, a, b, c, total):
        s1 = total[0, 0] + total[1, 0]
        s0 = total[0, 0] - total[1, 0]
        d1_ = total[0, 1] + total[1, 1]
        d0_ = total[0, 1] - total[1, 1]
        for i, s, d in ((0, s0, d0_), (1, s1, d1_)):
            for k, value in ((0, s - d), (1, s + d)):
                spot = at(n, a, b + i, c + k)
                if (i == 1 or b == 0) and (k == 1 or c == 0):
                    dst[spot] = value
                else:
                    dst[spot] += value

    def diagonal(level):
        n, h = cells[level], widths[level]
        dst, coeff = parts[level], coeffs[level]
        tiles = {}
        for a in range(n):
            for b in range(n):
                for c in range(n):
                    hx, hy, hz = h[a], h[b], h[c]
                    scale = hy * hz / (9 * hx) + hx * hz / (9 * hy) + hx * hy / (9 * hz)
                    tile = coeff[own(n, a + 1, b + 1, c + 1)] * scale
                    for i in range(2):
                        for j in range(2):
                            for k in range(2):
                                spot = at(n, a + i, b + j, c + k)
                                first = (i or a == 0) and (j or b == 0) and (k or c == 0)
                                if first:
                                    dst[spot] = tile
                                else:
                                    dst[spot] += tile
        fold(dst, n)
        for a, b, c in owned(n):
            diags[level][own(n, a, b, c)] = relax_weight / dst[at(n, a, b, c)]

    def pair_weights(level):
        h = widths[level]
        spans = [(h[2 * i], h[2 * i + 1]) for i in range(len(h) // 2)]
        return [q / (p + q) for p, q in spans], [p / (p + q) for p, q in spans]

    def restrict_to(level, defect, target):
        n = cells[level]
        m = n // 2
        left, right = pair_weights(level)

        def line(values, dim):
            result = []
            for o in range(1, m + 1):
                beyond = values[2 * o] if o < m else after(values[0], dim)
                result.append(
                    values[2 * o - 1] + right[o - 1] * values[2 * o - 2] + left[o % m] * beyond
                )
            return result

        slabs = []
        for a in range(1, n + 1):
            lines = [line([defect(a, b, c) for c in range(1, n + 1)], 2) for b in range(1, n + 1)]
            turned = [line([lines[b][c] for b in range(n)], 1) for c in range(m)]
            slabs.append(turned)
        for c in range(m):
            for b in range(m):
                out = line([slabs[a][c][b] for a in range(n)], 0)
                for a in range(m):
                    target[own(m, a + 1, b + 1, c + 1)] = inside(m, a + 1, b + 1, c + 1, out[a])

    def prolong_from(level, add):
        n = cells[level]
        m = n // 2
        left, right = pair_weights(level)
        src = fulls[level + 1]
        ghosts(src, m)

        def line(values):
            result = []
            for o in range(1, m + 1):
                result.append(left[o - 1] * values[o - 1] + right[o - 1] * values[o])
                result.append(values[o])
            return result

        slabs = []
        for a in range(m + 1):
            lines = [line([src[at(m, a, b, c)] for c in range(m + 1)]) for b in range(m + 1)]
            slabs.append([line([lines[b][c] for b in range(m + 1)]) for c in range(n)])
        for c in range(n):
            for b in range(n):
                out = line([slabs[a][c][b] for a in range(m + 1)])
                for a in range(n):
                    add(a + 1, b + 1, c + 1, out[a])

    def cycle_at(level, forcing, store):
        n = cells[level]
        src, dst, diag = fulls[level], parts[level], diags[level]
        for a, b, c in owned(n):
            spot = own(n, a, b, c)
            src[at(n, a, b, c)] = forcing[spot] * diag[spot]
        lor(level)
        if level < LEVELS - 1:
            restrict_to(
                level,
                lambda a, b, c: forcing[own(n, a, b, c)] - dst[at(n, a, b, c)],
                (f1, f2)[level],
            )

            def leave(a, b, c, tile):
                fulls[level + 1][at(n // 2, a, b, c)] = tile

            cycle_at(level + 1, (f1, f2)[level], leave)

            def add(a, b, c, tile):
                src[at(n, a, b, c)] += tile

            prolong_from(level, add)
            lor(level)
        for a, b, c in owned(n):
            spot = own(n, a, b, c)
            change = inside(n, a, b, c, (forcing[spot] - dst[at(n, a, b, c)]) * diag[spot])
            store(a, b, c, src[at(n, a, b, c)] + change)

    def derive(u):
        e = [u[0] + u[4], u[1] + u[3], u[2]]
        o = [u[0] - u[4], u[1] - u[3]]
        odd = []
        even = []
        for i in range(2):
            odd.append(sum(
                e[j] * float((deriv[i, j] + deriv[i, 4 - j]) / 2 if j < 2 else deriv[i, 2])
                for j in range(3)
            ))
        for i in range(3):
            even.append(sum(o[j] * float((deriv[i, j] - deriv[i, 4 - j]) / 2) for j in range(2)))
        return [even[0] + odd[0], even[1] + odd[1], even[2], even[1] - odd[1], even[0] - odd[0]]

    def derive_back(g):
        e = [g[0] + g[4], g[1] + g[3], g[2]]
        o = [g[0] - g[4], g[1] - g[3]]
        odd = []
        even = []
        for a in range(2):
            odd.append(sum(
                e[j] * float((deriv[j, a] + deriv[4 - j, a]) / 2 if j < 2 else deriv[2, a])
                for j in range(3)
            ))
        for a in range(3):
            even.append(sum(o[j] * float((deriv[j, a] - deriv[4 - j, a]) / 2) for j in range(2)))
        return [even[0] + odd[0], even[1] + odd[1], even[2], even[1] - odd[1], even[0] - odd[0]]

    def stiffness():
        ghosts(full, 4)

        def run(spots, first):
            grad = derive([full[s] for s in spots])
            back = derive_back([grad[i] * weighted[s] for i, s in enumerate(spots)])
            for s, value in zip(spots, back):
                if first:
                    part[s] = value
                else:
                    part[s] += value

        def outer(i, carry):
            for k in range(5):
                run([25 * i + 5 * k + t for t in range(5)], True)
            for k in range(5):
                run([25 * i + 5 * t + k for t in range(5)], False)
            return carry

        def along(i, carry):
            for k in range(5):
                run([25 * t + 5 * i + k for t in range(5)], False)
            return carry

        lax.fori_loop(0, 5, outer, 0)
        lax.fori_loop(0, 5, along, 0)
        fold(part, 4)

    for copy in copies:
        copy.wait()

    low = lane < lanes // 2
    for a in range(5):
        for b in range(5):
            for c in range(5):
                spot = 25 * a + 5 * b + c
                first = gathered[pl.ds(spot, rows, stride=stride), :]
                second = gathered[pl.ds(half + spot, rows, stride=stride), :]
                cube = float(quad[a] * quad[b] * quad[c])
                full[spot] = jnp.where(low, first, pltpu.roll(second, lanes // 2, 1))
                part[spot] = jnp.where(low, pltpu.roll(first, lanes // 2, 1), second) * cube
                weighted[spot] = full[spot] * cube
    fold(part, 4)
    for a, b, c in owned(4):
        resid[own(4, a, b, c)] = inside(4, a, b, c, part[at(4, a, b, c)])
    for a in range(4):
        for b in range(4):
            plane = [
                (full[at(4, a, b, c)] + full[at(4, a + 1, b, c)])
                + (full[at(4, a, b + 1, c)] + full[at(4, a + 1, b + 1, c)])
                for c in range(5)
            ]
            for c in range(4):
                c0[own(4, a + 1, b + 1, c + 1)] = (plane[c] + plane[c + 1]) * 0.125
    for level in range(LEVELS - 1):
        m = cells[level + 1]
        for a, b, c in owned(m):
            total = None
            for i in range(2):
                for j in range(2):
                    for k in range(2):
                        tile = coeffs[level][
                            own(2 * m, 2 * a - i, 2 * b - j, 2 * c - k)
                        ]
                        total = tile if total is None else total + tile
            coeffs[level + 1][own(m, a, b, c)] = total * 0.125
    for level in range(LEVELS):
        diagonal(level)

    direction[...] = jnp.zeros_like(direction)
    iterate[...] = jnp.zeros_like(iterate)

    def settle(a, b, c, tile):
        precond[own(4, a, b, c)] = tile

    def product(tiles):
        total = None
        for tile in tiles:
            total = tile if total is None else total + tile
        return jnp.sum(jnp.sum(total, axis=0, keepdims=True), axis=1, keepdims=True)

    def step(number, rho_old):
        cycle_at(0, resid, settle)
        rho = product(resid[i] * precond[i] for i in range(64))
        ratio = jnp.where(number == 0, 0.0, rho / rho_old)
        for a, b, c in owned(4):
            spot = own(4, a, b, c)
            value = precond[spot] + ratio * direction[spot]
            direction[spot] = value
            full[at(4, a, b, c)] = value
        stiffness()
        curv = None
        for a, b, c in owned(4):
            image = inside(4, a, b, c, part[at(4, a, b, c)])
            precond[own(4, a, b, c)] = image
            term = direction[own(4, a, b, c)] * image
            curv = term if curv is None else curv + term
        alpha = rho / product([curv])
        for i in range(64):
            iterate[i] += alpha * direction[i]
            resid[i] -= alpha * precond[i]
        return rho

    lax.fori_loop(0, 2, step, jnp.ones((1, 1), jnp.float32))

    row = at_x * ny + at_y
    start = at_z * (lanes // 2)
    width = x_out.shape[2]
    ez = lax.broadcasted_iota(jnp.int32, (lanes, width), 0)
    spot_z = lax.broadcasted_iota(jnp.int32, (lanes, width), 1)
    for out, ref in ((x_out, iterate), (r_out, resid)):
        total = jnp.zeros((16, width), jnp.float32)
        for c in range(4):
            pick = (spot_z == 4 * (ez - start) + c).astype(jnp.float32)
            lines = jnp.concatenate(
                [ref[4 * ab + c, pl.ds(row, 1), :] for ab in range(16)], axis=0
            )
            total = total + jnp.dot(
                lines, pick, precision=lax.Precision.HIGHEST,
                preferred_element_type=jnp.float32,
            )
        for a in range(4):
            out[a] = total[4 * a : 4 * a + 4]


def exchange_offsets(nx, ny):
    strips = [2 * d for d in (0, 1, 3, 2)[:ny]] if ny <= 4 else [2 * d for d in range(ny)]
    return [
        (strip, across)
        for strip in strips
        for across in [4 * ny * i + z for z in range(2) for i in range(nx // 2)]
    ]


def whole_body(kappa, source):
    axes = ("gx", "gy", "gz")
    nx, ny = lax.axis_size("gx"), lax.axis_size("gy")
    rows, lanes = nx * ny, 2 * kappa.shape[5]

    def swap(block, distance):
        return lax.ppermute(block, axes, [(i, i ^ distance) for i in range(2 * rows)])

    packed = jnp.concatenate([kappa.reshape(125, -1), source.reshape(125, -1)], axis=1)
    packed = jnp.pad(packed, ((0, 3), (0, 0)))
    offsets = exchange_offsets(nx, ny)
    strips = {}
    pieces = []
    for strip, across in offsets:
        if across == 0:
            strips[strip] = swap(packed, strip) if strip else packed
            pieces.append(strips[strip])
        elif across & 1 and across > 1:
            pieces.append(swap(strips[strip ^ across ^ 1], 1))
        else:
            strips[strip ^ across] = swap(strips[strip], across)
            pieces.append(strips[strip ^ across])
    near = jnp.stack(pieces)
    far = swap(near, 2 * ny)

    def tiles(count):
        return pltpu.VMEM((count, rows, lanes), jnp.float32)

    counts = [125, 125, 125, 64, 8, 1, 64, 8, 1, 8, 1, 27, 27, 8, 8, 64, 64, 64, 64]
    shape = jax.ShapeDtypeStruct((4, 4, 2 * lanes), jnp.float32)
    vmem = pl.BlockSpec(memory_space=pltpu.VMEM)
    anywhere = pl.BlockSpec(memory_space=pl.ANY)
    return tuple(pl.pallas_call(
        lambda *refs: iteration_kernel(
            *refs, ny=ny, offsets=[strip ^ across for strip, across in offsets]
        ),
        out_shape=(shape, shape),
        in_specs=[anywhere, anywhere],
        out_specs=(vmem, vmem),
        scratch_shapes=[tiles(n) for n in counts]
        + [pltpu.VMEM((2 * rows * 128, lanes), jnp.float32)]
        + [pltpu.SemaphoreType.DMA((2 * len(offsets),))],
        compiler_params=pltpu.CompilerParams(vmem_limit_bytes=40 * 2**20),
        name="whole_iteration",
    )(near, far))


def fits_whole(kappa, mesh):
    sizes = mesh.shape
    rows = sizes["gx"] * sizes["gy"]
    one_column = kappa.shape[3] == sizes["gx"] and kappa.shape[4] == sizes["gy"]
    lanes = kappa.shape[5]
    return (
        one_column
        and sizes["gz"] == 2
        and all(n & (n - 1) == 0 and n > 1 for n in (sizes["gx"], sizes["gy"]))
        and rows % 8 == 0
        and lanes % 128 == 0
        and rows * lanes <= 16 * 128
    )


def solution(mesh):
    placed = (P(None, None, None, "gx", "gy", "gz"), P(None, None, None, "gx", "gy", "gz"))

    def run(kappa, source):
        return jax.shard_map(
            whole_body if fits_whole(kappa, mesh) else body,
            mesh=mesh,
            in_specs=placed,
            out_specs=(P("gx", "gy", "gz"), P("gx", "gy", "gz")),
            check_vma=False,
        )(kappa, source)

    return run
```
